32 devices in a mesh: dp: 4 (over z), shard: 8 (over y, x, core).
Axes of the slice: x: 2, y: 2, z: 4, core: 2. Of those that a mesh axis runs over, the one named last changes fastest.
Arguments:
- gradients: bfloat16 [4, 2, 512, 16, 512], P('dp', None, 'shard'), may hold values from -6 to 6
- owner_list: int32 [32], replicated, may hold values from 0 to 31, as said below
- row_offset: int32 [32], replicated, may hold values from 0 to 512, as said below
- col_offset: int32 [32], replicated, may hold values from 0 to 7680, as said below
- left_factor: float32 [64, 512, 512], P(('dp', 'shard')), may hold values from -32 to 32, as said below
- right_factor: float32 [64, 512, 512], P(('dp', 'shard')), may hold values from -32 to 32, as said below
- left_root: float32 [64, 512, 512], P(('dp', 'shard')), may hold values from -2 to 2, as said below
- right_root: float32 [64, 512, 512], P(('dp', 'shard')), may hold values from -2 to 2, as said below
Outputs:
- update: bfloat16 [2, 512, 16, 512], P(None, 'shard', None, 'dp')
- new_left_factor: float32 [64, 512, 512], P(('dp', 'shard'))
- new_right_factor: float32 [64, 512, 512], P(('dp', 'shard'))
- new_left_root: float32 [64, 512, 512], P(('dp', 'shard'))
- new_right_root: float32 [64, 512, 512], P(('dp', 'shard'))
The draws below stay inside these ranges and needn't reach their ends.
Inputs may be any that keep to these rules, and one draw needn't show every extreme that they name: `owner_list`: no owner is named by more than 2 entries, and some owner by exactly 2. `row_offset`: multiples of 512; with col_offset, every block of the 2 x 16 grid is named exactly once. `col_offset`: multiples of 512; with row_offset, every block of the grid is named exactly once. `left_factor`: each slot symmetric positive definite. `right_factor`: each slot symmetric positive definite. `left_root`: each slot symmetric. `right_root`: each slot symmetric.
All inputs are finite; a program needn't handle non-finite values.
Results may differ from the reference program's by a relative error of at most 0.012.
Values may be sent and summed in bfloat16 or wider, within the bound.
A program may use at most 128 MiB of HBM per device.

```python
import jax
import jax.numpy as jnp
from jax import lax

BLOCK = 512
SLOTS = 2
REPLICAS = 4
BC = 16
BR = 2
BLOCKS = 32
SLOTS_ALL = 64


def draw_owner_list(key, part):
    base = jax.random.fold_in(key, 7)
    first_key, second_key, third_key = jax.random.split(base, 3)
    owner_count = SLOTS_ALL // SLOTS
    starred = jax.random.randint(first_key, (), 0, owner_count)
    others = jax.random.permutation(second_key, SLOTS_ALL - SLOTS).astype(jnp.int32)
    others = others + SLOTS * (others >= SLOTS * starred).astype(jnp.int32)
    rest = others[:BLOCKS - SLOTS] // SLOTS
    owners = jnp.concatenate([jnp.full((SLOTS,), starred, jnp.int32), rest.astype(jnp.int32)])
    shuffle = jax.random.permutation(third_key, BLOCKS)
    return owners[shuffle].astype(jnp.int32)


def grid_order(key):
    return jax.random.permutation(jax.random.fold_in(key, 11), BLOCKS).astype(jnp.int32)


def draw_row_offset(key, part):
    return (grid_order(key) // BC * BLOCK).astype(jnp.int32)


def draw_col_offset(key, part):
    return (grid_order(key) % BC * BLOCK).astype(jnp.int32)


def factor_draw(key):
    first_key = jax.random.fold_in(key, 0)
    noise = jax.random.normal(first_key, (SLOTS_ALL, BLOCK, BLOCK), jnp.float32)
    gram = jnp.einsum('nij,nkj->nik', noise, noise, precision=lax.Precision.HIGHEST) / BLOCK
    return gram + 0.5 * jnp.eye(BLOCK, dtype=jnp.float32)[None]


def draw_left_factor(key, part):
    return factor_draw(jax.random.fold_in(key, 3))


def draw_right_factor(key, part):
    return factor_draw(jax.random.fold_in(key, 5))


def root_draw(key):
    noise = jax.random.normal(key, (SLOTS_ALL, BLOCK, BLOCK), jnp.float32)
    symmetric = (noise + jnp.swapaxes(noise, 1, 2)) / (2.0 * BLOCK ** 0.5)
    return jnp.eye(BLOCK, dtype=jnp.float32)[None] + 0.3 * symmetric


def draw_left_root(key, part):
    return root_draw(jax.random.fold_in(key, 13))


def draw_right_root(key, part):
    return root_draw(jax.random.fold_in(key, 17))


def level_of(stream_key, shape, cuts, smallest, largest):
    loudness = 1.0
    for axis_at, shards_of in cuts:
        draws = jax.random.uniform(jax.random.fold_in(jax.random.fold_in(stream_key, 6), axis_at), (shards_of,), jnp.float32, smallest / len(cuts), largest / len(cuts))
        loudness = loudness * jnp.repeat(jnp.exp(draws), shape[axis_at] // shards_of).reshape((-1,) + (1,) * (len(shape) - 1 - axis_at))
    return loudness


def centred(own_key, shape, scale, reach, cuts=(), kind=jnp.bfloat16):
    loudness = level_of(own_key, shape, cuts, -0.22, 0.18) if cuts else 1.0
    drawn = jax.random.normal(own_key, shape, jnp.float32) * scale * loudness
    return jnp.minimum(jnp.maximum(drawn, -reach), reach).astype(kind)


def setup_inputs(seed: int = 0) -> dict:
    splits = jax.random.split(jax.random.key(seed), 9)
    gradients = centred(splits[0], (REPLICAS, BR, BLOCK, BC, BLOCK), 0.5, 6.0, ((0, 4), (2, 8)))
    owner_list = draw_owner_list(jax.random.fold_in(splits[8], 71), 0)
    row_offset = draw_row_offset(jax.random.fold_in(splits[8], 71), 0)
    col_offset = draw_col_offset(jax.random.fold_in(splits[8], 71), 0)
    left_factor = draw_left_factor(jax.random.fold_in(splits[8], 71), 0)
    right_factor = draw_right_factor(jax.random.fold_in(splits[8], 71), 0)
    left_root = draw_left_root(jax.random.fold_in(splits[8], 71), 0)
    right_root = draw_right_root(jax.random.fold_in(splits[8], 71), 0)
    return {"gradients": gradients, "owner_list": owner_list, "row_offset": row_offset, "col_offset": col_offset, "left_factor": left_factor, "right_factor": right_factor, "left_root": left_root, "right_root": right_root}


decay_rate = 0.9
highest = lax.Precision.HIGHEST


def newton_root(factor, old_root):
    identity = jnp.eye(factor.shape[0], dtype=factor.dtype)
    normed = factor * (factor.shape[0] / jnp.trace(factor))
    root_sq = jnp.dot(old_root, old_root, precision=highest)
    root_quad = jnp.dot(root_sq, root_sq, precision=highest)
    coupled = jnp.dot(root_quad, normed, precision=highest)
    newton_t = (5.0 * identity - coupled) / 4.0
    return jnp.dot(old_root, newton_t, precision=highest)


def per_block(inputs):
    g_block, left_old, right_old, left_prev, right_prev = inputs
    gram_left = jnp.dot(g_block, g_block.T, preferred_element_type=jnp.float32)
    gram_right = jnp.dot(g_block.T, g_block, preferred_element_type=jnp.float32)
    left_new = decay_rate * left_old + ((1.0 - decay_rate) / BLOCK) * gram_left
    right_new = decay_rate * right_old + ((1.0 - decay_rate) / BLOCK) * gram_right
    left_next = newton_root(left_new, left_prev)
    right_next = newton_root(right_new, right_prev)
    g_float = g_block.astype(jnp.float32)
    result = jnp.dot(jnp.dot(left_next, g_float, precision=highest), right_next, precision=highest)
    return result.astype(jnp.bfloat16), left_new, right_new, left_next, right_next


def reference(gradients, owner_list, row_offset, col_offset, left_factor, right_factor, left_root, right_root):
    summed = jnp.sum(gradients.astype(jnp.float32), axis=0).astype(jnp.bfloat16)
    block_row = (row_offset // BLOCK).astype(jnp.int32)
    block_col = (col_offset // BLOCK).astype(jnp.int32)
    entry_index = jnp.arange(BLOCKS, dtype=jnp.int32)
    same_owner = owner_list[None, :] == owner_list[:, None]
    earlier = jnp.sum(same_owner & (entry_index[None, :] < entry_index[:, None]), axis=1).astype(jnp.int32)
    slot_of = (owner_list * SLOTS + earlier).astype(jnp.int32)
    pieces = summed[block_row, :, block_col, :]
    outputs = lax.map(per_block, (pieces, left_factor[slot_of], right_factor[slot_of], left_root[slot_of], right_root[slot_of]))
    blocks_out, left_new, right_new, left_next, right_next = outputs
    update = jnp.zeros((BR, BLOCK, BC, BLOCK), jnp.bfloat16).at[block_row, :, block_col, :].set(blocks_out)
    new_left_factor = left_factor.at[slot_of].set(left_new)
    new_right_factor = right_factor.at[slot_of].set(right_new)
    new_left_root = left_root.at[slot_of].set(left_next)
    new_right_root = right_root.at[slot_of].set(right_next)
    return update, new_left_factor, new_right_factor, new_left_root, new_right_root
```

```python
import functools

import jax
import jax.numpy as jnp
from jax import lax
from jax.experimental import pallas as pl
from jax.experimental.pallas import tpu as pltpu
from jax.sharding import PartitionSpec as P

decay_rate = 0.9
MESH = pl.DeviceIdType.MESH
f32 = jnp.float32
bf16 = jnp.bfloat16


def split(x):
    hi = x.astype(bf16)
    return hi, (x - hi.astype(f32)).astype(bf16)


def mm(a, b, ca=1, cb=0):
    return lax.dot_general(a, b, (((ca,), (cb,)), ((), ())), preferred_element_type=f32)


def mm3(a, b):
    return mm(a[0], b[0]) + (mm(a[0], b[1]) + mm(a[1], b[0]))


def fifth_power(x):
    x = split(x)
    square = split(mm3(x, x))
    quad = split(mm3(square, square))
    return split(mm3(quad, x))


def root_of(factor, power, old_root):
    size = factor.shape[0]
    row = lax.broadcasted_iota(jnp.int32, factor.shape, 0)
    col = lax.broadcasted_iota(jnp.int32, factor.shape, 1)
    trace = jnp.sum(jnp.where(row == col, factor, 0.0))
    return 1.25 * old_root - mm3(power, split(factor)) * (size / (4.0 * trace))


def shampoo_kernel(n, sh, slots, table_ref, grad_ref, lf_hbm, rf_hbm, lr_hbm, rr_hbm,
                   out_ref, nlf_ref, nrf_ref, nlr_ref, nrr_ref,
                   own, from_left, from_right, acc, pieces, packed, g_ref, u_ref, returned,
                   factors, roots, powers,
                   load_sem, factor_sem, root_sem, send_sem, left_sem, right_sem,
                   out_sem, in_sem, back_out_sem, back_in_sem):
    me = lax.axis_index("dp")
    shard = lax.axis_index("shard")
    total = n * sh
    parts, rows, cols, width = own.shape[1:]
    size = g_ref.shape[1]
    blocks = parts * cols
    index = me * sh + shard
    loads = {}
    order = []
    for j in range(n):
        for t in (n - 1 - j, j):
            if t not in order:
                order.append(t)
    for t in order:
        for b in range(parts):
            loads[t, b] = pltpu.make_async_copy(
                grad_ref.at[0, b, :, :, pl.ds(t * width, width)], own.at[t, b], load_sem.at[t, b]
            )
            loads[t, b].start()
    root_loads = [
        pltpu.make_async_copy(ref, roots.at[i], root_sem.at[i])
        for i, ref in enumerate((lr_hbm, rr_hbm))
    ]
    factor_loads = [
        pltpu.make_async_copy(ref, factors.at[i], factor_sem.at[i])
        for i, ref in enumerate((lf_hbm, rf_hbm))
    ]
    for copy in root_loads + factor_loads:
        copy.start()
    barrier = pltpu.get_barrier_semaphore()

    @pl.loop(1, total)
    def _(r):
        to = lax.rem(index + r, total)
        pl.semaphore_signal(
            barrier, inc=1, device_id=(to // sh, lax.rem(to, sh)), device_id_type=MESH
        )

    for t in order:
        for b in range(parts):
            loads[t, b].wait()
    pl.semaphore_wait(barrier, total - 1)

    def hop(t, b, step):
        buffer, sem = (from_left, left_sem) if step > 0 else (from_right, right_sem)
        return pltpu.make_async_remote_copy(
            src_ref=own.at[t, b],
            dst_ref=buffer.at[t, b],
            send_sem=send_sem.at[t, b],
            recv_sem=sem.at[t, b],
            device_id=(me + step, shard),
            device_id_type=MESH,
        )

    units = [(i, s) for s in range(slots) for i in range(2)]

    def next_power():
        if units:
            i, s = units.pop(0)
            hi, lo = fifth_power(roots[i, s])
            powers[i, 0, s] = hi
            powers[i, 1, s] = lo

    def first_hop(t, b, step):
        hop(t, b, step).start()

    def pass_on(t, b, step):
        hop(t, b, step).wait_recv()
        buffer = from_left if step > 0 else from_right
        own[t, b] = (own[t, b].astype(f32) + buffer[t, b].astype(f32)).astype(bf16)
        hop(t, b, step).start()

    hops = [
        (t, b, step)
        for j in range(n - 1)
        for b in range(parts)
        for t, step in ((n - 1 - j, 1), (j, -1))
    ]
    for t, b, step in hops:
        pl.when(me == (0 if step > 0 else n - 1))(functools.partial(first_hop, t, b, step))
    for copy in root_loads:
        copy.wait()
    next_power()
    every = max(1, 2 * parts // 2)
    for k, (t, b, step) in enumerate(hops):
        inner = (me < t) & (me > 0) if step > 0 else (me > t) & (me < n - 1)
        pl.when(inner)(functools.partial(pass_on, t, b, step))
        if k % every == every - 1:
            next_power()
    while units:
        next_power()
    for copy in factor_loads:
        copy.wait()
    for b in range(parts):
        acc[b] = own[me, b].astype(f32)

        @pl.when(me > 0)
        def _():
            hop(me, b, 1).wait_recv()
            acc[b] += from_left[me, b].astype(f32)

        @pl.when(me < n - 1)
        def _():
            hop(me, b, -1).wait_recv()
            acc[b] += from_right[me, b].astype(f32)

        for c in range(cols):
            pieces[b * cols + c] = acc[b, :, c, :].astype(bf16)

    my_rows = pl.ds(pl.multiple_of(shard * rows, rows), rows)
    my_cols = pl.ds(pl.multiple_of(me * width, width), width)

    def peers(visit):
        for dz in sorted(range(n), key=lambda d: abs(2 * d - n)):
            @pl.loop(0 if dz else 1, sh)
            def _(ds):
                visit(lax.rem(me + dz, n), lax.rem(shard + ds, sh))

    def forward(slot):
        @pl.loop(0, total)
        def _(d):
            packed[slot, d] = pieces[table_ref[d * slots + slot]]

        def send(z, s):
            pltpu.make_async_remote_copy(
                src_ref=packed.at[slot, z * sh + s],
                dst_ref=g_ref.at[slot, my_rows, my_cols],
                send_sem=out_sem.at[slot],
                recv_sem=in_sem.at[slot],
                device_id=(z, s),
                device_id_type=MESH,
            ).start()

        peers(send)
        g_ref[slot, my_rows, my_cols] = packed[slot, index]

    def backward(slot):
        def send(z, s):
            pltpu.make_async_remote_copy(
                src_ref=u_ref.at[
                    slot,
                    pl.ds(pl.multiple_of(s * rows, rows), rows),
                    pl.ds(pl.multiple_of(z * width, width), width),
                ],
                dst_ref=returned.at[index * slots + slot],
                send_sem=back_out_sem.at[slot],
                recv_sem=back_in_sem.at[slot],
                device_id=(z, s),
                device_id_type=MESH,
            ).start()

        peers(send)
        returned[index * slots + slot] = u_ref[slot, my_rows, my_cols]

    def wait_all(sem):
        ref = packed.at[0, pl.ds(0, total - 1)]
        pltpu.make_async_copy(ref, ref, sem).wait()

    count = table_ref[total * slots + blocks]
    rate = (1.0 - decay_rate) / size

    def step(slot):
        live = slot < count
        g = g_ref[slot]
        left_old, right_old = factors[0, slot], factors[1, slot]
        left = decay_rate * left_old + rate * mm(g, g, 1, 1)
        right = decay_rate * right_old + rate * mm(g, g, 0, 0)
        nlf_ref[slot] = jnp.where(live, left, left_old)
        nrf_ref[slot] = jnp.where(live, right, right_old)
        left_root = root_of(left, (powers[0, 0, slot], powers[0, 1, slot]), roots[0, slot])
        nlr_ref[slot] = jnp.where(live, left_root, roots[0, slot])
        right_root = root_of(right, (powers[1, 0, slot], powers[1, 1, slot]), roots[1, slot])
        nrr_ref[slot] = jnp.where(live, right_root, roots[1, slot])
        hi, lo = split(left_root)
        product = split(mm(hi, g) + mm(lo, g))
        u_ref[slot] = mm3(product, split(right_root)).astype(bf16)

    for slot in range(slots):
        forward(slot)
    for slot in range(slots):
        wait_all(in_sem.at[slot])
        step(slot)
        backward(slot)
    for slot in range(slots):
        wait_all(back_in_sem.at[slot])
    for b in range(parts):
        for c in range(cols):
            acc[b, :, c, :] = returned[table_ref[total * slots + b * cols + c]].astype(f32)
        out_ref[b] = acc[b].astype(bf16)
    for slot in range(slots):
        wait_all(out_sem.at[slot])
        wait_all(back_out_sem.at[slot])
    for t in range(n):
        for b in range(parts):

            @pl.when(me != t)
            def _():
                hop(t, b, 1).wait_send()


def body(
    gradients, owner_list, row_offset, col_offset, left_factor, right_factor, left_root, right_root
):
    dp = lax.axis_size("dp")
    sh = lax.axis_size("shard")
    slots, size, _ = left_factor.shape
    _, parts, rows, cols, _ = gradients.shape
    width = size // dp
    total = dp * sh
    blocks = owner_list.shape[0]
    block_at = row_offset // size * cols + col_offset // size
    entry_index = jnp.arange(blocks, dtype=jnp.int32)
    same_owner = owner_list[None, :] == owner_list[:, None]
    earlier = jnp.sum(same_owner & (entry_index[None, :] < entry_index[:, None]), axis=1)
    slot_of = owner_list * slots + earlier
    slot_index = jnp.arange(total * slots, dtype=jnp.int32)
    block_of_slot = jnp.sum(
        jnp.where(slot_of[None, :] == slot_index[:, None], block_at[None, :], 0), axis=1
    )
    slot_of_block = jnp.sum(
        jnp.where(block_at[None, :] == entry_index[:, None], slot_of[None, :], 0), axis=1
    )
    my_index = lax.axis_index(("dp", "shard"))
    my_count = jnp.sum((owner_list == my_index).astype(jnp.int32), keepdims=True)
    table = jnp.concatenate([block_of_slot, slot_of_block, my_count]).astype(jnp.int32)

    smem = pl.BlockSpec(memory_space=pltpu.SMEM)
    vmem = pl.BlockSpec(memory_space=pltpu.VMEM)
    hbm = pl.BlockSpec(memory_space=pl.ANY)
    chunk = (dp, parts, rows, cols, width)
    matrices = (slots, size, size)
    dma = pltpu.SemaphoreType.DMA
    full = jax.ShapeDtypeStruct(matrices, f32)
    return pl.pallas_call(
        functools.partial(shampoo_kernel, dp, sh, slots),
        out_shape=[jax.ShapeDtypeStruct((parts, rows, cols, width), bf16)] + [full] * 4,
        in_specs=[smem] + [hbm] * 5,
        out_specs=[vmem] * 5,
        scratch_shapes=[
            pltpu.VMEM(chunk, bf16),
            pltpu.VMEM(chunk, bf16),
            pltpu.VMEM(chunk, bf16),
            pltpu.VMEM(chunk[1:], f32),
            pltpu.VMEM((parts * cols, rows, width), bf16),
            pltpu.VMEM((slots, total, rows, width), bf16),
            pltpu.VMEM(matrices, bf16),
            pltpu.VMEM(matrices, bf16),
            pltpu.VMEM((total * slots, rows, width), bf16),
            pltpu.VMEM((2,) + matrices, f32),
            pltpu.VMEM((2,) + matrices, f32),
            pltpu.VMEM((2, 2) + matrices, bf16),
            dma((dp, parts)), dma((2,)), dma((2,)),
            dma((dp, parts)), dma((dp, parts)), dma((dp, parts)),
            dma((slots,)), dma((slots,)), dma((slots,)), dma((slots,)),
        ],
        compiler_params=pltpu.CompilerParams(
            collective_id=0, has_side_effects=True, vmem_limit_bytes=60 * 2**20
        ),
        name="shampoo",
    )(table, gradients, left_factor, right_factor, left_root, right_root)


def solution(mesh):
    owned = P(("dp", "shard"), None, None)
    in_specs = (P("dp", None, "shard", None, None), P(), P(), P(), owned, owned, owned, owned)
    out_specs = (P(None, "shard", None, "dp"), owned, owned, owned, owned)
    return jax.shard_map(body, mesh=mesh, in_specs=in_specs, out_specs=out_specs, check_vma=False)
```

```python
import functools

import jax
import jax.numpy as jnp
from jax import lax
from jax.experimental import pallas as pl
from jax.experimental.pallas import tpu as pltpu
from jax.sharding import PartitionSpec as P

decay_rate = 0.9
MESH = pl.DeviceIdType.MESH
f32 = jnp.float32
bf16 = jnp.bfloat16


def split(x):
    hi = x.astype(bf16)
    return hi, (x - hi.astype(f32)).astype(bf16)


def mm(a, b, ca=1, cb=0):
    return lax.dot_general(a, b, (((ca,), (cb,)), ((), ())), preferred_element_type=f32)


def mm3(a, b):
    return mm(a[0], b[0]) + (mm(a[0], b[1]) + mm(a[1], b[0]))


def fifth_power(x):
    x = split(x)
    square = split(mm3(x, x))
    quad = split(mm3(square, square))
    return split(mm3(quad, x))


def root_of(factor, power, old_root):
    size = factor.shape[0]
    row = lax.broadcasted_iota(jnp.int32, factor.shape, 0)
    col = lax.broadcasted_iota(jnp.int32, factor.shape, 1)
    trace = jnp.sum(jnp.where(row == col, factor, 0.0))
    return 1.25 * old_root - mm3(power, split(factor)) * (size / (4.0 * trace))


def shampoo_kernel(n, sh, slots, table_ref, grad_ref, lf_hbm, rf_hbm, lr_hbm, rr_hbm,
                   returned, nlf_ref, nrf_ref, nlr_ref, nrr_ref,
                   own, from_left, from_right, acc, pieces, packed, g_ref, u_ref,
                   factors, roots, powers,
                   load_sem, factor_sem, root_sem, send_sem, left_sem, right_sem,
                   out_sem, in_sem, back_out_sem, back_in_sem):
    me = lax.axis_index("dp")
    shard = lax.axis_index("shard")
    total = n * sh
    parts, rows, cols, width = own.shape[1:]
    size = g_ref.shape[1]
    blocks = parts * cols
    index = me * sh + shard
    loads = {}
    order = []
    for j in range(n):
        for t in (n - 1 - j, j):
            if t not in order:
                order.append(t)
    for t in order:
        for b in range(parts):
            loads[t, b] = pltpu.make_async_copy(
                grad_ref.at[0, b, :, :, pl.ds(t * width, width)], own.at[t, b], load_sem.at[t, b]
            )
            loads[t, b].start()
    root_loads = [
        pltpu.make_async_copy(ref, roots.at[i], root_sem.at[i])
        for i, ref in enumerate((lr_hbm, rr_hbm))
    ]
    factor_loads = [
        pltpu.make_async_copy(ref, factors.at[i], factor_sem.at[i])
        for i, ref in enumerate((lf_hbm, rf_hbm))
    ]
    for copy in root_loads + factor_loads:
        copy.start()
    barrier = pltpu.get_barrier_semaphore()

    @pl.loop(1, total)
    def _(r):
        to = lax.rem(index + r, total)
        pl.semaphore_signal(
            barrier, inc=1, device_id=(to // sh, lax.rem(to, sh)), device_id_type=MESH
        )

    for t in order:
        for b in range(parts):
            loads[t, b].wait()
    pl.semaphore_wait(barrier, total - 1)

    def hop(t, b, step):
        buffer, sem = (from_left, left_sem) if step > 0 else (from_right, right_sem)
        return pltpu.make_async_remote_copy(
            src_ref=own.at[t, b],
            dst_ref=buffer.at[t, b],
            send_sem=send_sem.at[t, b],
            recv_sem=sem.at[t, b],
            device_id=(me + step, shard),
            device_id_type=MESH,
        )

    units = [(i, s) for s in range(slots) for i in range(2)]

    def next_power():
        if units:
            i, s = units.pop(0)
            hi, lo = fifth_power(roots[i, s])
            powers[i, 0, s] = hi
            powers[i, 1, s] = lo

    def first_hop(t, b, step):
        hop(t, b, step).start()

    def pass_on(t, b, step):
        hop(t, b, step).wait_recv()
        buffer = from_left if step > 0 else from_right
        own[t, b] = (own[t, b].astype(f32) + buffer[t, b].astype(f32)).astype(bf16)
        hop(t, b, step).start()

    hops = [
        (t, b, step)
        for j in range(n - 1)
        for b in range(parts)
        for t, step in ((n - 1 - j, 1), (j, -1))
    ]
    for t, b, step in hops:
        pl.when(me == (0 if step > 0 else n - 1))(functools.partial(first_hop, t, b, step))
    for copy in root_loads:
        copy.wait()
    next_power()
    every = max(1, 2 * parts // 2)
    for k, (t, b, step) in enumerate(hops):
        inner = (me < t) & (me > 0) if step > 0 else (me > t) & (me < n - 1)
        pl.when(inner)(functools.partial(pass_on, t, b, step))
        if k % every == every - 1:
            next_power()
    while units:
        next_power()
    for copy in factor_loads:
        copy.wait()
    for b in range(parts):
        acc[b] = own[me, b].astype(f32)

        @pl.when(me > 0)
        def _():
            hop(me, b, 1).wait_recv()
            acc[b] += from_left[me, b].astype(f32)

        @pl.when(me < n - 1)
        def _():
            hop(me, b, -1).wait_recv()
            acc[b] += from_right[me, b].astype(f32)

        for c in range(cols):
            pieces[b * cols + c] = acc[b, :, c, :].astype(bf16)

    my_rows = pl.ds(pl.multiple_of(shard * rows, rows), rows)
    my_cols = pl.ds(pl.multiple_of(me * width, width), width)

    def peers(visit):
        for dz in sorted(range(n), key=lambda d: abs(2 * d - n)):
            @pl.loop(0 if dz else 1, sh)
            def _(ds):
                visit(lax.rem(me + dz, n), lax.rem(shard + ds, sh))

    def forward(slot):
        @pl.loop(0, total)
        def _(d):
            packed[slot, d] = pieces[table_ref[d * slots + slot]]

        def send(z, s):
            pltpu.make_async_remote_copy(
                src_ref=packed.at[slot, z * sh + s],
                dst_ref=g_ref.at[slot, my_rows, my_cols],
                send_sem=out_sem.at[slot],
                recv_sem=in_sem.at[slot],
                device_id=(z, s),
                device_id_type=MESH,
            ).start()

        peers(send)
        g_ref[slot, my_rows, my_cols] = packed[slot, index]

    def backward(slot):
        def send(z, s):
            pltpu.make_async_remote_copy(
                src_ref=u_ref.at[
                    slot,
                    pl.ds(pl.multiple_of(s * rows, rows), rows),
                    pl.ds(pl.multiple_of(z * width, width), width),
                ],
                dst_ref=returned.at[index * slots + slot],
                send_sem=back_out_sem.at[slot],
                recv_sem=back_in_sem.at[slot],
                device_id=(z, s),
                device_id_type=MESH,
            ).start()

        peers(send)
        returned[index * slots + slot] = u_ref[slot, my_rows, my_cols]

    def wait_all(sem):
        ref = packed.at[0, pl.ds(0, total - 1)]
        pltpu.make_async_copy(ref, ref, sem).wait()

    count = table_ref[total * slots + blocks]
    rate = (1.0 - decay_rate) / size

    def step(slot):
        live = slot < count
        g = g_ref[slot]
        left_old, right_old = factors[0, slot], factors[1, slot]
        left = decay_rate * left_old + rate * mm(g, g, 1, 1)
        right = decay_rate * right_old + rate * mm(g, g, 0, 0)
        nlf_ref[slot] = jnp.where(live, left, left_old)
        nrf_ref[slot] = jnp.where(live, right, right_old)
        left_root = root_of(left, (powers[0, 0, slot], powers[0, 1, slot]), roots[0, slot])
        nlr_ref[slot] = jnp.where(live, left_root, roots[0, slot])
        right_root = root_of(right, (powers[1, 0, slot], powers[1, 1, slot]), roots[1, slot])
        nrr_ref[slot] = jnp.where(live, right_root, roots[1, slot])
        hi, lo = split(left_root)
        product = split(mm(hi, g) + mm(lo, g))
        u_ref[slot] = mm3(product, split(right_root)).astype(bf16)

    for slot in range(slots):
        forward(slot)
    for slot in range(slots):
        wait_all(in_sem.at[slot])
        step(slot)
        backward(slot)
    for slot in range(slots):
        wait_all(back_in_sem.at[slot])
    for slot in range(slots):
        wait_all(out_sem.at[slot])
        wait_all(back_out_sem.at[slot])
    for t in range(n):
        for b in range(parts):

            @pl.when(me != t)
            def _():
                hop(t, b, 1).wait_send()


def place_kernel(first, table_ref, returned, *refs):
    news, out_ref, outs = refs[:4], refs[4], refs[5:9]
    acc, sems = refs[9:]
    copies = [
        pltpu.make_async_copy(new, out, sems.at[i])
        for i, (new, out) in enumerate(zip(news, outs))
    ]
    for copy in copies:
        copy.start()
    parts, _, cols, _ = out_ref.shape
    for b in range(parts):
        for c in range(cols):
            acc[b, :, c, :] = returned[table_ref[first + b * cols + c]].astype(f32)
        out_ref[b] = acc[b].astype(bf16)
    for copy in copies:
        copy.wait()


def body(
    gradients, owner_list, row_offset, col_offset, left_factor, right_factor, left_root, right_root
):
    dp = lax.axis_size("dp")
    sh = lax.axis_size("shard")
    slots, size, _ = left_factor.shape
    _, parts, rows, cols, _ = gradients.shape
    width = size // dp
    total = dp * sh
    blocks = owner_list.shape[0]
    block_at = row_offset // size * cols + col_offset // size
    entry_index = jnp.arange(blocks, dtype=jnp.int32)
    same_owner = owner_list[None, :] == owner_list[:, None]
    earlier = jnp.sum(same_owner & (entry_index[None, :] < entry_index[:, None]), axis=1)
    slot_of = owner_list * slots + earlier
    slot_index = jnp.arange(total * slots, dtype=jnp.int32)
    block_of_slot = jnp.sum(
        jnp.where(slot_of[None, :] == slot_index[:, None], block_at[None, :], 0), axis=1
    )
    slot_of_block = jnp.sum(
        jnp.where(block_at[None, :] == entry_index[:, None], slot_of[None, :], 0), axis=1
    )
    my_index = lax.axis_index(("dp", "shard"))
    my_count = jnp.sum((owner_list == my_index).astype(jnp.int32), keepdims=True)
    table = jnp.concatenate([block_of_slot, slot_of_block, my_count]).astype(jnp.int32)

    smem = pl.BlockSpec(memory_space=pltpu.SMEM)
    vmem = pl.BlockSpec(memory_space=pltpu.VMEM)
    hbm = pl.BlockSpec(memory_space=pltpu.HBM)
    chunk = (dp, parts, rows, cols, width)
    matrices = (slots, size, size)
    dma = pltpu.SemaphoreType.DMA
    full = jax.ShapeDtypeStruct(matrices, f32)
    pieces = (total * slots, rows, width)
    returned, *news = pl.pallas_call(
        functools.partial(shampoo_kernel, dp, sh, slots),
        out_shape=[pltpu.VMEM(pieces, bf16)] + [pltpu.VMEM(matrices, f32)] * 4,
        in_specs=[smem] + [hbm] * 5,
        out_specs=[vmem] * 5,
        scratch_shapes=[
            pltpu.VMEM(chunk, bf16),
            pltpu.VMEM(chunk, bf16),
            pltpu.VMEM(chunk, bf16),
            pltpu.VMEM(chunk[1:], f32),
            pltpu.VMEM((parts * cols, rows, width), bf16),
            pltpu.VMEM((slots, total, rows, width), bf16),
            pltpu.VMEM(matrices, bf16),
            pltpu.VMEM(matrices, bf16),
            pltpu.VMEM((2,) + matrices, f32),
            pltpu.VMEM((2,) + matrices, f32),
            pltpu.VMEM((2, 2) + matrices, bf16),
            dma((dp, parts)), dma((2,)), dma((2,)),
            dma((dp, parts)), dma((dp, parts)), dma((dp, parts)),
            dma((slots,)), dma((slots,)), dma((slots,)), dma((slots,)),
        ],
        compiler_params=pltpu.CompilerParams(
            collective_id=0, has_side_effects=True, vmem_limit_bytes=48 * 2**20
        ),
        name="shampoo",
    )(table, gradients, left_factor, right_factor, left_root, right_root)
    return pl.pallas_call(
        functools.partial(place_kernel, total * slots),
        out_shape=[jax.ShapeDtypeStruct((parts, rows, cols, width), bf16)] + [full] * 4,
        in_specs=[smem] + [vmem] * 5,
        out_specs=[vmem] + [hbm] * 4,
        scratch_shapes=[pltpu.VMEM((parts, rows, cols, width), f32), dma((4,))],
        compiler_params=pltpu.CompilerParams(vmem_limit_bytes=16 * 2**20),
        name="place",
    )(table, returned, *news)


def solution(mesh):
    owned = P(("dp", "shard"), None, None)
    in_specs = (P("dp", None, "shard", None, None), P(), P(), P(), owned, owned, owned, owned)
    out_specs = (P(None, "shard", None, "dp"), owned, owned, owned, owned)
    return jax.shard_map(body, mesh=mesh, in_specs=in_specs, out_specs=out_specs, check_vma=False)
```

```python
import functools

import jax
import jax.numpy as jnp
from jax import lax
from jax.experimental import pallas as pl
from jax.experimental.pallas import tpu as pltpu
from jax.sharding import PartitionSpec as P

decay_rate = 0.9
MESH = pl.DeviceIdType.MESH
f32 = jnp.float32
bf16 = jnp.bfloat16


def split(x):
    hi = x.astype(bf16)
    return hi, (x - hi.astype(f32)).astype(bf16)


def mm(a, b, ca=1, cb=0):
    return lax.dot_general(a, b, (((ca,), (cb,)), ((), ())), preferred_element_type=f32)


def mm3(a, b):
    return mm(a[0], b[0]) + (mm(a[0], b[1]) + mm(a[1], b[0]))


def fifth_power(x):
    x = split(x)
    square = split(mm3(x, x))
    quad = split(mm3(square, square))
    return split(mm3(quad, x))


def root_of(factor, power, old_root):
    size = factor.shape[0]
    row = lax.broadcasted_iota(jnp.int32, factor.shape, 0)
    col = lax.broadcasted_iota(jnp.int32, factor.shape, 1)
    trace = jnp.sum(jnp.where(row == col, factor, 0.0))
    return 1.25 * old_root - mm3(power, split(factor)) * (size / (4.0 * trace))


def arrivals(n, parts):
    events = {me: [] for me in range(n)}
    for step in (1, -1):
        line = list(range(n))[::step]
        ready = {(t, b): 0 for t in line[:0:-1] for b in range(parts)}
        for k, me in enumerate(line[:-1]):
            free = 0
            for (t, b), at in sorted(ready.items(), key=lambda item: item[1]):
                if t in line[:k + 1]:
                    continue
                events[me].append((at, t, b, step))
                free = ready[t, b] = max(free, at) + 1
    return events


def build_table(index, slots, cols, size, owner_ref, row_ref, col_ref, table):
    blocks = owner_ref.shape[1]
    square = (blocks, blocks)
    row = lax.broadcasted_iota(jnp.int32, square, 0)
    col = lax.broadcasted_iota(jnp.int32, square, 1)

    def upright(x):
        return jnp.sum(jnp.where(row == col, x, 0), axis=1, keepdims=True)

    def total(pick, x):
        return jnp.sum(jnp.where(pick, x, 0), axis=0, keepdims=True)

    shift = size.bit_length() - 1
    owner = owner_ref[...]
    slot = owner * slots + total((upright(owner) == owner) & (row < col), 1)
    block = lax.shift_right_logical(row_ref[...], shift) * cols
    block = block + lax.shift_right_logical(col_ref[...], shift)
    slot, block = upright(slot), upright(block)
    lanes = table.shape[1]
    lane = lax.broadcasted_iota(jnp.int32, (blocks, lanes), 1)
    table[0:1] = total(slot == lane, block)
    table[1:2] = total(block == lane, slot)
    table[2:3] = total(upright(owner) == index, jnp.ones((blocks, lanes), jnp.int32))


def shampoo_kernel(n, sh, slots, owner_ref, row_ref, col_ref, grad_ref, lf_hbm, rf_hbm, lr_hbm, rr_hbm,
                   table, returned, nlf_ref, nrf_ref, nlr_ref, nrr_ref,
                   own, from_left, from_right, acc, pieces, packed, g_ref, u_ref, table_ref,
                   factors, roots, powers,
                   load_sem, table_sem, factor_sem, root_sem, send_sem, left_sem, right_sem,
                   out_sem, in_sem, back_out_sem, back_in_sem):
    me = lax.axis_index("dp")
    shard = lax.axis_index("shard")
    total = n * sh
    parts, rows, cols, width = own.shape[1:]
    size = g_ref.shape[1]
    index = me * sh + shard
    loads = {}
    order = []
    for j in range(n):
        for t in (n - 1 - j, j):
            if t not in order:
                order.append(t)
    for t in order:
        for b in range(parts):
            loads[t, b] = pltpu.make_async_copy(
                grad_ref.at[0, b, :, :, pl.ds(t * width, width)], own.at[t, b], load_sem.at[t, b]
            )
            loads[t, b].start()
    root_loads = [
        pltpu.make_async_copy(ref, roots.at[i], root_sem.at[i])
        for i, ref in enumerate((lr_hbm, rr_hbm))
    ]
    factor_loads = [
        pltpu.make_async_copy(ref, factors.at[i], factor_sem.at[i])
        for i, ref in enumerate((lf_hbm, rf_hbm))
    ]
    for copy in root_loads + factor_loads:
        copy.start()
    barrier = pltpu.get_barrier_semaphore()

    @pl.loop(1, total)
    def _(r):
        to = lax.rem(index + r, total)
        pl.semaphore_signal(
            barrier, inc=1, device_id=(to // sh, lax.rem(to, sh)), device_id_type=MESH
        )

    for t in order:
        for b in range(parts):
            loads[t, b].wait()
    pl.semaphore_wait(barrier, total - 1)

    def hop(t, b, step):
        buffer, sem = (from_left, left_sem) if step > 0 else (from_right, right_sem)
        return pltpu.make_async_remote_copy(
            src_ref=own.at[t, b],
            dst_ref=buffer.at[t, b],
            send_sem=send_sem.at[t, b],
            recv_sem=sem.at[t, b],
            device_id=(me + step, shard),
            device_id_type=MESH,
        )

    units = [(i, s) for s in range(slots) for i in range(2)]

    def next_power():
        if units:
            i, s = units.pop(0)
            hi, lo = fifth_power(roots[i, s])
            powers[i, 0, s] = hi
            powers[i, 1, s] = lo

    def first_hop(t, b, step):
        hop(t, b, step).start()

    def pass_on(t, b, step):
        hop(t, b, step).wait_recv()
        buffer = from_left if step > 0 else from_right
        own[t, b] = (own[t, b].astype(f32) + buffer[t, b].astype(f32)).astype(bf16)
        hop(t, b, step).start()

    events = arrivals(n, parts)
    for end in (0, n - 1):

        @pl.when(me == end)
        def _():
            for _, t, b, step in events[end]:
                first_hop(t, b, step)

    build_table(index, slots, cols, size, owner_ref, row_ref, col_ref, table)
    table_copy = pltpu.make_async_copy(table, table_ref, table_sem)
    table_copy.start()
    for copy in root_loads:
        copy.wait()
    next_power()
    last = max(at for k in range(1, n - 1) for at, *_ in events[k])
    for now in range(1, last + 1):
        for k in range(1, n - 1):
            arriving = [event for event in events[k] if event[0] == now]
            if arriving:

                @pl.when(me == k)
                def _():
                    for _, t, b, step in arriving:
                        pass_on(t, b, step)

        next_power()
    while units:
        next_power()
    table_copy.wait()
    for copy in factor_loads:
        copy.wait()
    for b in range(parts):
        acc[b] = own[me, b].astype(f32)

        @pl.when(me > 0)
        def _():
            hop(me, b, 1).wait_recv()
            acc[b] += from_left[me, b].astype(f32)

        @pl.when(me < n - 1)
        def _():
            hop(me, b, -1).wait_recv()
            acc[b] += from_right[me, b].astype(f32)

        for c in range(cols):
            pieces[b * cols + c] = acc[b, :, c, :].astype(bf16)

    my_rows = pl.ds(pl.multiple_of(shard * rows, rows), rows)
    my_cols = pl.ds(pl.multiple_of(me * width, width), width)

    def peers(visit):
        for dz in sorted(range(n), key=lambda d: abs(2 * d - n)):
            @pl.loop(0 if dz else 1, sh)
            def _(ds):
                visit(lax.rem(me + dz, n), lax.rem(shard + ds, sh))

    def forward(slot):
        @pl.loop(0, total)
        def _(d):
            packed[slot, d] = pieces[table_ref[0, d * slots + slot]]

        def send(z, s):
            pltpu.make_async_remote_copy(
                src_ref=packed.at[slot, z * sh + s],
                dst_ref=g_ref.at[slot, my_rows, my_cols],
                send_sem=out_sem.at[slot],
                recv_sem=in_sem.at[slot],
                device_id=(z, s),
                device_id_type=MESH,
            ).start()

        peers(send)
        g_ref[slot, my_rows, my_cols] = packed[slot, index]

    def backward(slot):
        def send(z, s):
            pltpu.make_async_remote_copy(
                src_ref=u_ref.at[
                    slot,
                    pl.ds(pl.multiple_of(s * rows, rows), rows),
                    pl.ds(pl.multiple_of(z * width, width), width),
                ],
                dst_ref=returned.at[index * slots + slot],
                send_sem=back_out_sem.at[slot],
                recv_sem=back_in_sem.at[slot],
                device_id=(z, s),
                device_id_type=MESH,
            ).start()

        peers(send)
        returned[index * slots + slot] = u_ref[slot, my_rows, my_cols]

    def wait_all(sem):
        ref = packed.at[0, pl.ds(0, total - 1)]
        pltpu.make_async_copy(ref, ref, sem).wait()

    count = table_ref[2, 0]
    rate = (1.0 - decay_rate) / size

    def step(slot):
        live = slot < count
        g = g_ref[slot]
        left_old, right_old = factors[0, slot], factors[1, slot]
        left = decay_rate * left_old + rate * mm(g, g, 1, 1)
        right = decay_rate * right_old + rate * mm(g, g, 0, 0)
        nlf_ref[slot] = jnp.where(live, left, left_old)
        nrf_ref[slot] = jnp.where(live, right, right_old)
        left_root = root_of(left, (powers[0, 0, slot], powers[0, 1, slot]), roots[0, slot])
        nlr_ref[slot] = jnp.where(live, left_root, roots[0, slot])
        right_root = root_of(right, (powers[1, 0, slot], powers[1, 1, slot]), roots[1, slot])
        nrr_ref[slot] = jnp.where(live, right_root, roots[1, slot])
        hi, lo = split(left_root)
        product = split(mm(hi, g) + mm(lo, g))
        u_ref[slot] = mm3(product, split(right_root)).astype(bf16)

    for slot in range(slots):
        forward(slot)
    for slot in range(slots):
        wait_all(in_sem.at[slot])
        step(slot)
        backward(slot)
    for slot in range(slots):
        wait_all(back_in_sem.at[slot])
    for slot in range(slots):
        wait_all(out_sem.at[slot])
        wait_all(back_out_sem.at[slot])
    for t in range(n):
        for b in range(parts):

            @pl.when(me != t)
            def _():
                hop(t, b, 1).wait_send()


def place_kernel(table, returned, *refs):
    news, out_ref, outs = refs[:4], refs[4], refs[5:9]
    acc, table_ref, table_sem, sems = refs[9:]
    table_copy = pltpu.make_async_copy(table, table_ref, table_sem)
    table_copy.start()
    copies = [
        pltpu.make_async_copy(new, out, sems.at[i])
        for i, (new, out) in enumerate(zip(news, outs))
    ]
    for copy in copies:
        copy.start()
    parts, _, cols, _ = out_ref.shape
    table_copy.wait()
    for b in range(parts):
        for c in range(cols):
            acc[b, :, c, :] = returned[table_ref[1, b * cols + c]].astype(f32)
        out_ref[b] = acc[b].astype(bf16)
    for copy in copies:
        copy.wait()


def body(
    gradients, owner_list, row_offset, col_offset, left_factor, right_factor, left_root, right_root
):
    dp = lax.axis_size("dp")
    sh = lax.axis_size("shard")
    slots, size, _ = left_factor.shape
    _, parts, rows, cols, _ = gradients.shape
    width = size // dp
    total = dp * sh
    blocks = owner_list.shape[0]
    lanes = -(-max(total * slots, blocks) // 128) * 128
    rowed = [x.reshape(1, blocks) for x in (owner_list, row_offset, col_offset)]

    vmem = pl.BlockSpec(memory_space=pltpu.VMEM)
    hbm = pl.BlockSpec(memory_space=pltpu.HBM)
    chunk = (dp, parts, rows, cols, width)
    matrices = (slots, size, size)
    dma = pltpu.SemaphoreType.DMA
    full = jax.ShapeDtypeStruct(matrices, f32)
    pieces = (total * slots, rows, width)
    table, returned, *news = pl.pallas_call(
        functools.partial(shampoo_kernel, dp, sh, slots),
        out_shape=[pltpu.VMEM((8, lanes), jnp.int32), pltpu.VMEM(pieces, bf16)] + [pltpu.VMEM(matrices, f32)] * 4,
        in_specs=[vmem] * 3 + [hbm] * 5,
        out_specs=[vmem] * 6,
        scratch_shapes=[
            pltpu.VMEM(chunk, bf16),
            pltpu.VMEM(chunk, bf16),
            pltpu.VMEM(chunk, bf16),
            pltpu.VMEM(chunk[1:], f32),
            pltpu.VMEM((parts * cols, rows, width), bf16),
            pltpu.VMEM((slots, total, rows, width), bf16),
            pltpu.VMEM(matrices, bf16),
            pltpu.VMEM(matrices, bf16),
            pltpu.SMEM((8, lanes), jnp.int32),
            pltpu.VMEM((2,) + matrices, f32),
            pltpu.VMEM((2,) + matrices, f32),
            pltpu.VMEM((2, 2) + matrices, bf16),
            dma((dp, parts)), dma, dma((2,)), dma((2,)),
            dma((dp, parts)), dma((dp, parts)), dma((dp, parts)),
            dma((slots,)), dma((slots,)), dma((slots,)), dma((slots,)),
        ],
        compiler_params=pltpu.CompilerParams(
            collective_id=0, has_side_effects=True, vmem_limit_bytes=48 * 2**20
        ),
        name="shampoo",
    )(*rowed, gradients, left_factor, right_factor, left_root, right_root)
    return pl.pallas_call(
        place_kernel,
        out_shape=[jax.ShapeDtypeStruct((parts, rows, cols, width), bf16)] + [full] * 4,
        in_specs=[vmem] * 6,
        out_specs=[vmem] + [hbm] * 4,
        scratch_shapes=[
            pltpu.VMEM((parts, rows, cols, width), f32),
            pltpu.SMEM((8, lanes), jnp.int32),
            dma, dma((4,)),
        ],
        compiler_params=pltpu.CompilerParams(vmem_limit_bytes=16 * 2**20),
        name="place",
    )(table, returned, *news)


def solution(mesh):
    owned = P(("dp", "shard"), None, None)
    in_specs = (P("dp", None, "shard", None, None), P(), P(), P(), owned, owned, owned, owned)
    out_specs = (P(None, "shard", None, "dp"), owned, owned, owned, owned)
    return jax.shard_map(body, mesh=mesh, in_specs=in_specs, out_specs=out_specs, check_vma=False)
```

```python
import functools

import jax
import jax.numpy as jnp
from jax import lax
from jax.experimental import pallas as pl
from jax.experimental.pallas import tpu as pltpu
from jax.sharding import PartitionSpec as P

decay_rate = 0.9
MESH = pl.DeviceIdType.MESH
f32 = jnp.float32
bf16 = jnp.bfloat16


def split(x):
    hi = x.astype(bf16)
    return hi, (x - hi.astype(f32)).astype(bf16)


def mm(a, b, ca=1, cb=0):
    return lax.dot_general(a, b, (((ca,), (cb,)), ((), ())), preferred_element_type=f32)


def mm3(a, b):
    return mm(a[0], b[0]) + (mm(a[0], b[1]) + mm(a[1], b[0]))


def root_of(factor, power, old_root):
    size = factor.shape[0]
    row = lax.broadcasted_iota(jnp.int32, factor.shape, 0)
    col = lax.broadcasted_iota(jnp.int32, factor.shape, 1)
    trace = jnp.sum(jnp.where(row == col, factor, 0.0))
    return 1.25 * old_root - mm3(power, split(factor)) * (size / (4.0 * trace))


def share_out(n, rows):
    tall = 32 if rows % 32 == 0 else rows
    cells = [(q, r) for q in range(n) for r in range(0, rows, tall)]
    shares = [len(cells) // n] * n
    if n == 4 and len(cells) % 8 == 0:
        shares = [len(cells) * 3 // 8, len(cells) // 8, len(cells) // 8, len(cells) * 3 // 8]
    starts = [sum(shares[:me]) for me in range(n)]
    return tall, [cells[at:at + share] for at, share in zip(starts, shares)]


def runs_of(cells, tall):
    runs = []
    for k, (q, r) in enumerate(cells):
        if runs and runs[-1][1] == q:
            runs[-1][3] += tall
        else:
            runs.append([k * tall, q, r, tall])
    return runs


def arrivals(owned, parts, latency=0.75):
    n = len(owned)
    events = {me: [] for me in range(n)}
    finals = {me: {} for me in range(n)}
    for step in (1, -1):
        line = list(range(n))[::step]
        ready = {(q, r, b, t): 0 for t in line[:0:-1] for q, r in owned[t] for b in range(parts)}
        for me in line:
            free = 0
            for chunk, at in sorted(ready.items(), key=lambda item: item[1]):
                if chunk[3] == me:
                    finals[me][chunk] = max(finals[me].get(chunk, 0), at)
                    del ready[chunk]
                else:
                    events[me].append((at, chunk, step))
                    free = max(free, at) + 1
                    ready[chunk] = free + latency
    return events, {me: sorted(finals[me], key=finals[me].get) for me in range(n)}


def build_table(index, slots, cols, size, owner_ref, row_ref, col_ref, table):
    blocks = owner_ref.shape[1]
    square = (blocks, blocks)
    row = lax.broadcasted_iota(jnp.int32, square, 0)
    col = lax.broadcasted_iota(jnp.int32, square, 1)

    def upright(x):
        return jnp.sum(jnp.where(row == col, x, 0), axis=1, keepdims=True)

    def total(pick, x):
        return jnp.sum(jnp.where(pick, x, 0), axis=0, keepdims=True)

    shift = size.bit_length() - 1
    owner = owner_ref[...]
    slot = owner * slots + total((upright(owner) == owner) & (row < col), 1)
    block = lax.shift_right_logical(row_ref[...], shift) * cols
    block = block + lax.shift_right_logical(col_ref[...], shift)
    slot, block = upright(slot), upright(block)
    lanes = table.shape[1]
    lane = lax.broadcasted_iota(jnp.int32, (blocks, lanes), 1)
    table[0:1] = total(slot == lane, block)
    table[1:2] = total(block == lane, slot)
    table[2:3] = total(upright(owner) == index, jnp.ones((blocks, lanes), jnp.int32))


def shampoo_kernel(n, sh, slots, owner_ref, row_ref, col_ref, grad_ref, lf_hbm, rf_hbm, lr_hbm, rr_hbm,
                   table, returned, nlf_ref, nrf_ref, nlr_ref, nrr_ref,
                   own, from_left, from_right, acc, pieces, packed, g_ref, u_ref, table_ref,
                   factors, roots, powers,
                   load_sem, table_sem, factor_sem, root_sem, send_sem, left_sem, right_sem,
                   out_sem, in_sem, back_out_sem, back_in_sem):
    me = lax.axis_index("dp")
    shard = lax.axis_index("shard")
    total = n * sh
    parts, rows, cols, width = own.shape[1:]
    size = g_ref.shape[1]
    tall, owned = share_out(n, rows)
    events, finals = arrivals(owned, parts)
    chunks = [(q, r, b, t) for t in range(n) for q, r in owned[t] for b in range(parts)]
    index = me * sh + shard
    loads = {}
    order = []
    for j in range(n):
        for t in (n - 1 - j, j):
            if t not in order:
                order.append(t)
    for t in order:
        for b in range(parts):
            loads[t, b] = pltpu.make_async_copy(
                grad_ref.at[0, b, :, :, pl.ds(t * width, width)], own.at[t, b], load_sem.at[t, b]
            )
            loads[t, b].start()
    root_loads = [
        pltpu.make_async_copy(ref, roots.at[i], root_sem.at[i])
        for i, ref in enumerate((lr_hbm, rr_hbm))
    ]
    factor_loads = [
        pltpu.make_async_copy(ref, factors.at[i], factor_sem.at[i])
        for i, ref in enumerate((lf_hbm, rf_hbm))
    ]
    for copy in root_loads + factor_loads:
        copy.start()
    barrier = pltpu.get_barrier_semaphore()

    @pl.loop(1, total)
    def _(r):
        to = lax.rem(index + r, total)
        pl.semaphore_signal(
            barrier, inc=1, device_id=(to // sh, lax.rem(to, sh)), device_id_type=MESH
        )

    for t in order:
        for b in range(parts):
            loads[t, b].wait()
    pl.semaphore_wait(barrier, total - 1)

    def place_of(chunk):
        q, r, b, _ = chunk
        return (q, b, pl.ds(r, tall)), (q, r // tall, b)

    def hop(chunk, step):
        buffer, sem = (from_left, left_sem) if step > 0 else (from_right, right_sem)
        at, sem_at = place_of(chunk)
        return pltpu.make_async_remote_copy(
            src_ref=own.at[at],
            dst_ref=buffer.at[at],
            send_sem=send_sem.at[sem_at],
            recv_sem=sem.at[sem_at],
            device_id=(me + step, shard),
            device_id_type=MESH,
        )

    units = [(i, s, part) for s in range(slots) for i in range(2) for part in range(3)]

    def next_power():
        if units:
            i, s, part = units.pop(0)
            if part == 0:
                x = split(roots[i, s])
                result = mm3(x, x)
            else:
                x = (powers[i, 0, s], powers[i, 1, s])
                result = mm3(x, x if part == 1 else split(roots[i, s]))
            powers[i, 0, s], powers[i, 1, s] = split(result)

    def pass_on(chunk, step):
        hop(chunk, step).wait_recv()
        buffer = from_left if step > 0 else from_right
        at, _ = place_of(chunk)
        own[at] = (own[at].astype(f32) + buffer[at].astype(f32)).astype(bf16)
        hop(chunk, step).start()

    def finish(k, chunk):
        at, _ = place_of(chunk)
        value = own[at].astype(f32)
        if k > 0:
            hop(chunk, 1).wait_recv()
            value = value + from_left[at].astype(f32)
        if k < n - 1:
            hop(chunk, -1).wait_recv()
            value = value + from_right[at].astype(f32)
        q, r, b, _ = chunk
        acc[...] = value
        first = owned[k].index((q, r)) * tall
        for c in range(cols):
            pieces[b * cols + c, first:first + tall] = acc[:, c, :].astype(bf16)

    def by_plane(visit):
        for k in range(n):
            pl.when(me == k)(functools.partial(visit, k))

    for end in (0, n - 1):

        @pl.when(me == end)
        def _():
            for _, chunk, step in events[end]:
                hop(chunk, step).start()

    build_table(index, slots, cols, size, owner_ref, row_ref, col_ref, table)
    table_copy = pltpu.make_async_copy(table, table_ref, table_sem)
    table_copy.start()
    for copy in root_loads:
        copy.wait()
    next_power()
    next_power()
    times = sorted({at for k in range(1, n - 1) for at, *_ in events[k]})
    pace = -(-len(units) // max(1, len(times) - 1))
    for now in times:
        for k in range(1, n - 1):
            arriving = [event for event in events[k] if event[0] == now]
            if arriving:

                @pl.when(me == k)
                def _():
                    for _, chunk, step in arriving:
                        pass_on(chunk, step)

        for _ in range(pace):
            next_power()
    while units:
        next_power()
    table_copy.wait()
    for copy in factor_loads:
        copy.wait()

    @by_plane
    def _(k):
        for chunk in finals[k]:
            finish(k, chunk)

    my_rows = pl.ds(pl.multiple_of(shard * rows, rows), rows)
    my_cols = pl.ds(pl.multiple_of(me * width, width), width)

    def peers(visit):
        for dz in sorted(range(n), key=lambda d: abs(2 * d - n)):
            @pl.loop(0 if dz else 1, sh)
            def _(ds):
                visit(lax.rem(me + dz, n), lax.rem(shard + ds, sh))

    def forward(slot, k):
        tops = len(owned[k]) * tall

        @pl.loop(0, total)
        def _(d):
            packed[slot, d, 0:tops] = pieces[table_ref[0, d * slots + slot], 0:tops]

        def block_part(q, r, high):
            return (
                slot,
                pl.ds(pl.multiple_of(shard * rows + r, tall), high),
                pl.ds(q * width, width),
            )

        def send(z, s):
            for top, q, r, high in runs_of(owned[k], tall):
                pltpu.make_async_remote_copy(
                    src_ref=packed.at[slot, z * sh + s, pl.ds(top, high)],
                    dst_ref=g_ref.at[block_part(q, r, high)],
                    send_sem=out_sem.at[slot],
                    recv_sem=in_sem.at[slot],
                    device_id=(z, s),
                    device_id_type=MESH,
                ).start()

        peers(send)
        for top, q, r, high in runs_of(owned[k], tall):
            g_ref[block_part(q, r, high)] = packed[slot, index, pl.ds(top, high)]

    def wait_forward(slot, k):
        incoming = n * (size // tall) - len(owned[k])
        ref = returned.at[pl.ds(0, incoming), pl.ds(0, tall)]
        pltpu.make_async_copy(ref, ref, in_sem.at[slot]).wait()

    def wait_forward_sent(slot, k):
        ref = packed.at[slot, pl.ds(0, total - 1), pl.ds(0, len(owned[k]) * tall)]
        pltpu.make_async_copy(ref, ref, out_sem.at[slot]).wait()

    def backward(slot):
        def send(z, s):
            pltpu.make_async_remote_copy(
                src_ref=u_ref.at[
                    slot,
                    pl.ds(pl.multiple_of(s * rows, rows), rows),
                    pl.ds(pl.multiple_of(z * width, width), width),
                ],
                dst_ref=returned.at[index * slots + slot],
                send_sem=back_out_sem.at[slot],
                recv_sem=back_in_sem.at[slot],
                device_id=(z, s),
                device_id_type=MESH,
            ).start()

        peers(send)
        returned[index * slots + slot] = u_ref[slot, my_rows, my_cols]

    def wait_return(sem):
        ref = returned.at[pl.ds(0, total - 1)]
        pltpu.make_async_copy(ref, ref, sem).wait()

    count = table_ref[2, 0]
    rate = (1.0 - decay_rate) / size

    def step(slot):
        live = slot < count
        g = g_ref[slot]
        left_old, right_old = factors[0, slot], factors[1, slot]
        left = decay_rate * left_old + rate * mm(g, g, 1, 1)
        right = decay_rate * right_old + rate * mm(g, g, 0, 0)
        nlf_ref[slot] = jnp.where(live, left, left_old)
        nrf_ref[slot] = jnp.where(live, right, right_old)
        left_root = root_of(left, (powers[0, 0, slot], powers[0, 1, slot]), roots[0, slot])
        nlr_ref[slot] = jnp.where(live, left_root, roots[0, slot])
        right_root = root_of(right, (powers[1, 0, slot], powers[1, 1, slot]), roots[1, slot])
        nrr_ref[slot] = jnp.where(live, right_root, roots[1, slot])
        hi, lo = split(left_root)
        product = split(mm(hi, g) + mm(lo, g))
        u_ref[slot] = mm3(product, split(right_root)).astype(bf16)

    @by_plane
    def _(k):
        for slot in range(slots):
            forward(slot, k)

    for slot in range(slots):
        by_plane(functools.partial(wait_forward, slot))
        step(slot)
        backward(slot)
    for slot in range(slots):
        wait_return(back_in_sem.at[slot])
        wait_return(back_out_sem.at[slot])
        by_plane(functools.partial(wait_forward_sent, slot))
    for chunk in chunks:

        @pl.when(me != chunk[3])
        def _():
            hop(chunk, 1).wait_send()


def place_kernel(table, returned, *refs):
    news, out_ref, outs = refs[:4], refs[4], refs[5:9]
    acc, table_ref, table_sem, sems = refs[9:]
    table_copy = pltpu.make_async_copy(table, table_ref, table_sem)
    table_copy.start()
    copies = [
        pltpu.make_async_copy(new, out, sems.at[i])
        for i, (new, out) in enumerate(zip(news, outs))
    ]
    for copy in copies:
        copy.start()
    parts, _, cols, _ = out_ref.shape
    table_copy.wait()
    for b in range(parts):
        for c in range(cols):
            acc[b, :, c, :] = returned[table_ref[1, b * cols + c]].astype(f32)
        out_ref[b] = acc[b].astype(bf16)
    for copy in copies:
        copy.wait()


def body(
    gradients, owner_list, row_offset, col_offset, left_factor, right_factor, left_root, right_root
):
    dp = lax.axis_size("dp")
    sh = lax.axis_size("shard")
    slots, size, _ = left_factor.shape
    _, parts, rows, cols, _ = gradients.shape
    width = size // dp
    total = dp * sh
    blocks = owner_list.shape[0]
    tall, owned = share_out(dp, rows)
    held = max(len(cells) for cells in owned) * tall
    hops = (dp, rows // tall, parts)
    lanes = -(-max(total * slots, blocks) // 128) * 128
    rowed = [x.reshape(1, blocks) for x in (owner_list, row_offset, col_offset)]

    vmem = pl.BlockSpec(memory_space=pltpu.VMEM)
    hbm = pl.BlockSpec(memory_space=pltpu.HBM)
    chunk = (dp, parts, rows, cols, width)
    matrices = (slots, size, size)
    dma = pltpu.SemaphoreType.DMA
    full = jax.ShapeDtypeStruct(matrices, f32)
    pieces = (total * slots, rows, width)
    table, returned, *news = pl.pallas_call(
        functools.partial(shampoo_kernel, dp, sh, slots),
        out_shape=[pltpu.VMEM((8, lanes), jnp.int32), pltpu.VMEM(pieces, bf16)] + [pltpu.VMEM(matrices, f32)] * 4,
        in_specs=[vmem] * 3 + [hbm] * 5,
        out_specs=[vmem] * 6,
        scratch_shapes=[
            pltpu.VMEM(chunk, bf16),
            pltpu.VMEM(chunk, bf16),
            pltpu.VMEM(chunk, bf16),
            pltpu.VMEM((tall, cols, width), f32),
            pltpu.VMEM((parts * cols, held, width), bf16),
            pltpu.VMEM((slots, total, held, width), bf16),
            pltpu.VMEM(matrices, bf16),
            pltpu.VMEM(matrices, bf16),
            pltpu.SMEM((8, lanes), jnp.int32),
            pltpu.VMEM((2,) + matrices, f32),
            pltpu.VMEM((2,) + matrices, f32),
            pltpu.VMEM((2, 2) + matrices, bf16),
            dma((dp, parts)), dma, dma((2,)), dma((2,)),
            dma(hops), dma(hops), dma(hops),
            dma((slots,)), dma((slots,)), dma((slots,)), dma((slots,)),
        ],
        compiler_params=pltpu.CompilerParams(
            collective_id=0, has_side_effects=True, vmem_limit_bytes=48 * 2**20
        ),
        name="shampoo",
    )(*rowed, gradients, left_factor, right_factor, left_root, right_root)
    return pl.pallas_call(
        place_kernel,
        out_shape=[jax.ShapeDtypeStruct((parts, rows, cols, width), bf16)] + [full] * 4,
        in_specs=[vmem] * 6,
        out_specs=[vmem] + [hbm] * 4,
        scratch_shapes=[
            pltpu.VMEM((parts, rows, cols, width), f32),
            pltpu.SMEM((8, lanes), jnp.int32),
            dma, dma((4,)),
        ],
        compiler_params=pltpu.CompilerParams(vmem_limit_bytes=16 * 2**20),
        name="place",
    )(table, returned, *news)


def solution(mesh):
    owned = P(("dp", "shard"), None, None)
    in_specs = (P("dp", None, "shard", None, None), P(), P(), P(), owned, owned, owned, owned)
    out_specs = (P(None, "shard", None, "dp"), owned, owned, owned, owned)
    return jax.shard_map(body, mesh=mesh, in_specs=in_specs, out_specs=out_specs, check_vma=False)
```

```python
import functools

import jax
import jax.numpy as jnp
from jax import lax
from jax.experimental import pallas as pl
from jax.experimental.pallas import tpu as pltpu
from jax.sharding import PartitionSpec as P

decay_rate = 0.9
MESH = pl.DeviceIdType.MESH
f32 = jnp.float32
bf16 = jnp.bfloat16


def split(x):
    hi = x.astype(bf16)
    return hi, (x - hi.astype(f32)).astype(bf16)


def mm(a, b, ca=1, cb=0):
    return lax.dot_general(a, b, (((ca,), (cb,)), ((), ())), preferred_element_type=f32)


def mm3(a, b):
    return mm(a[0], b[0]) + (mm(a[0], b[1]) + mm(a[1], b[0]))


def root_of(factor, power, old_root):
    size = factor.shape[0]
    row = lax.broadcasted_iota(jnp.int32, factor.shape, 0)
    col = lax.broadcasted_iota(jnp.int32, factor.shape, 1)
    trace = jnp.sum(jnp.where(row == col, factor, 0.0))
    return 1.25 * old_root - mm3(power, split(factor)) * (size / (4.0 * trace))


def share_out(n, rows):
    tall = 32 if rows % 32 == 0 else rows
    cells = [(q, r) for q in range(n) for r in range(0, rows, tall)]
    shares = [len(cells) // n] * n
    if n == 4 and len(cells) % 8 == 0:
        shares = [len(cells) * 3 // 8, len(cells) // 8, len(cells) // 8, len(cells) * 3 // 8]
    starts = [sum(shares[:me]) for me in range(n)]
    return tall, [cells[at:at + share] for at, share in zip(starts, shares)]


def runs_of(cells, tall):
    runs = []
    for k, (q, r) in enumerate(cells):
        if runs and runs[-1][1] == q:
            runs[-1][3] += tall
        else:
            runs.append([k * tall, q, r, tall])
    return runs


def arrivals(owned, parts, latency=0.75):
    n = len(owned)
    events = {me: [] for me in range(n)}
    finals = {me: {} for me in range(n)}
    for step in (1, -1):
        line = list(range(n))[::step]
        ready = {(q, r, b, t): 0 for t in line[:0:-1] for q, r in owned[t] for b in range(parts)}
        for me in line:
            free = 0
            for chunk, at in sorted(ready.items(), key=lambda item: item[1]):
                if chunk[3] == me:
                    finals[me][chunk] = max(finals[me].get(chunk, 0), at)
                    del ready[chunk]
                else:
                    events[me].append((at, chunk, step))
                    free = max(free, at) + 1
                    ready[chunk] = free + latency
    return events, {me: sorted(finals[me], key=finals[me].get) for me in range(n)}


def build_table(index, slots, cols, size, owner_ref, row_ref, col_ref, table):
    blocks = owner_ref.shape[1]
    square = (blocks, blocks)
    row = lax.broadcasted_iota(jnp.int32, square, 0)
    col = lax.broadcasted_iota(jnp.int32, square, 1)

    def upright(x):
        return jnp.sum(jnp.where(row == col, x, 0), axis=1, keepdims=True)

    def total(pick, x):
        return jnp.sum(jnp.where(pick, x, 0), axis=0, keepdims=True)

    shift = size.bit_length() - 1
    owner = owner_ref[...]
    slot = owner * slots + total((upright(owner) == owner) & (row < col), 1)
    block = lax.shift_right_logical(row_ref[...], shift) * cols
    block = block + lax.shift_right_logical(col_ref[...], shift)
    slot, block = upright(slot), upright(block)
    lanes = table.shape[1]
    lane = lax.broadcasted_iota(jnp.int32, (blocks, lanes), 1)
    table[0:1] = total(slot == lane, block)
    table[1:2] = total(block == lane, slot)
    table[2:3] = total(upright(owner) == index, jnp.ones((blocks, lanes), jnp.int32))


def shampoo_kernel(n, sh, slots, owner_ref, row_ref, col_ref, grad_ref, lf_hbm, rf_hbm, lr_hbm, rr_hbm,
                   table, returned, nlf_ref, nrf_ref, nlr_ref, nrr_ref,
                   own, from_left, from_right, acc, pieces, packed, g_ref, u_ref, table_ref,
                   factors, roots, powers,
                   load_sem, table_sem, factor_sem, root_sem, send_sem, left_sem, right_sem,
                   out_sem, in_sem, back_out_sem, back_in_sem):
    me = lax.axis_index("dp")
    shard = lax.axis_index("shard")
    total = n * sh
    parts, rows, cols, width = own.shape[1:]
    size = g_ref.shape[1]
    tall, owned = share_out(n, rows)
    events, finals = arrivals(owned, parts)
    chunks = [(q, r, b, t) for t in range(n) for q, r in owned[t] for b in range(parts)]
    index = me * sh + shard
    barrier = pltpu.get_barrier_semaphore()

    @pl.loop(1, total)
    def _(r):
        to = lax.rem(index + r, total)
        pl.semaphore_signal(
            barrier, inc=1, device_id=(to // sh, lax.rem(to, sh)), device_id_type=MESH
        )

    loads = {}
    order = []
    for j in range(n):
        for t in (n - 1 - j, j):
            if t not in order:
                order.append(t)
    for t in order:
        for b in range(parts):
            loads[t, b] = pltpu.make_async_copy(
                grad_ref.at[0, b, :, :, pl.ds(t * width, width)], own.at[t, b], load_sem.at[t, b]
            )
            loads[t, b].start()
    root_loads = [
        pltpu.make_async_copy(ref, roots.at[i], root_sem.at[i])
        for i, ref in enumerate((lr_hbm, rr_hbm))
    ]
    factor_loads = [
        pltpu.make_async_copy(ref, factors.at[i], factor_sem.at[i])
        for i, ref in enumerate((lf_hbm, rf_hbm))
    ]
    for copy in root_loads + factor_loads:
        copy.start()
    for t in order:
        for b in range(parts):
            loads[t, b].wait()
    pl.semaphore_wait(barrier, total - 1)

    def place_of(chunk):
        q, r, b, _ = chunk
        return (q, b, pl.ds(r, tall)), (q, r // tall, b)

    def hop(chunk, step):
        buffer, sem = (from_left, left_sem) if step > 0 else (from_right, right_sem)
        at, sem_at = place_of(chunk)
        return pltpu.make_async_remote_copy(
            src_ref=own.at[at],
            dst_ref=buffer.at[at],
            send_sem=send_sem.at[sem_at],
            recv_sem=sem.at[sem_at],
            device_id=(me + step, shard),
            device_id_type=MESH,
        )

    units = [(i, s, part) for s in range(slots) for i in range(2) for part in range(3)]

    def next_power():
        if units:
            i, s, part = units.pop(0)
            if part == 0:
                x = split(roots[i, s])
                result = mm3(x, x)
            else:
                x = (powers[i, 0, s], powers[i, 1, s])
                result = mm3(x, x if part == 1 else split(roots[i, s]))
            powers[i, 0, s], powers[i, 1, s] = split(result)

    def pass_on(chunk, step):
        hop(chunk, step).wait_recv()
        buffer = from_left if step > 0 else from_right
        at, _ = place_of(chunk)
        own[at] = (own[at].astype(f32) + buffer[at].astype(f32)).astype(bf16)
        hop(chunk, step).start()

    def finish(k, chunk):
        at, _ = place_of(chunk)
        value = own[at].astype(f32)
        if k > 0:
            hop(chunk, 1).wait_recv()
            value = value + from_left[at].astype(f32)
        if k < n - 1:
            hop(chunk, -1).wait_recv()
            value = value + from_right[at].astype(f32)
        q, r, b, _ = chunk
        acc[...] = value
        first = owned[k].index((q, r)) * tall
        for c in range(cols):
            pieces[b * cols + c, first:first + tall] = acc[:, c, :].astype(bf16)

    def by_plane(visit):
        for k in range(n):
            pl.when(me == k)(functools.partial(visit, k))

    for end in (0, n - 1):

        @pl.when(me == end)
        def _():
            for _, chunk, step in events[end]:
                hop(chunk, step).start()

    build_table(index, slots, cols, size, owner_ref, row_ref, col_ref, table)
    table_copy = pltpu.make_async_copy(table, table_ref, table_sem)
    table_copy.start()
    for copy in root_loads:
        copy.wait()
    next_power()
    next_power()
    times = sorted({at for k in range(1, n - 1) for at, *_ in events[k]})
    pace = -(-len(units) // max(1, len(times) - 1))
    for now in times:
        for k in range(1, n - 1):
            arriving = [event for event in events[k] if event[0] == now]
            if arriving:

                @pl.when(me == k)
                def _():
                    for _, chunk, step in arriving:
                        pass_on(chunk, step)

        for _ in range(pace):
            next_power()
    while units:
        next_power()
    table_copy.wait()
    for copy in factor_loads:
        copy.wait()

    @by_plane
    def _(k):
        for chunk in finals[k]:
            finish(k, chunk)

    my_rows = pl.ds(pl.multiple_of(shard * rows, rows), rows)
    my_cols = pl.ds(pl.multiple_of(me * width, width), width)

    def planes_from(k):
        return sorted(range(n), key=lambda z: ((2 * z < n) == (2 * k < n), -abs(z - k)))

    def peers(k, z, visit):
        @pl.loop(1 if z == k else 0, sh)
        def _(ds):
            visit(z, lax.rem(shard + ds, sh))

    def forward(slot, k):
        tops = len(owned[k]) * tall

        def pack(z):
            @pl.loop(0, sh)
            def _(s):
                d = z * sh + s
                packed[slot, d, 0:tops] = pieces[table_ref[0, d * slots + slot], 0:tops]

        def block_part(q, r, high):
            return (
                slot,
                pl.ds(pl.multiple_of(shard * rows + r, tall), high),
                pl.ds(q * width, width),
            )

        def send(z, s):
            for top, q, r, high in runs_of(owned[k], tall):
                pltpu.make_async_remote_copy(
                    src_ref=packed.at[slot, z * sh + s, pl.ds(top, high)],
                    dst_ref=g_ref.at[block_part(q, r, high)],
                    send_sem=out_sem.at[slot],
                    recv_sem=in_sem.at[slot],
                    device_id=(z, s),
                    device_id_type=MESH,
                ).start()

        planes = planes_from(k)
        pack(planes[0])
        for z, following in zip(planes, planes[1:] + [None]):
            if following is not None:
                pack(following)
            peers(k, z, send)
        for top, q, r, high in runs_of(owned[k], tall):
            g_ref[block_part(q, r, high)] = packed[slot, index, pl.ds(top, high)]

    def wait_forward(slot, k):
        incoming = n * (size // tall) - len(owned[k])
        ref = returned.at[pl.ds(0, incoming), pl.ds(0, tall)]
        pltpu.make_async_copy(ref, ref, in_sem.at[slot]).wait()

    def wait_forward_sent(slot, k):
        ref = packed.at[slot, pl.ds(0, total - 1), pl.ds(0, len(owned[k]) * tall)]
        pltpu.make_async_copy(ref, ref, out_sem.at[slot]).wait()

    def backward(slot, k):
        def send(z, s):
            pltpu.make_async_remote_copy(
                src_ref=u_ref.at[
                    slot,
                    pl.ds(pl.multiple_of(s * rows, rows), rows),
                    pl.ds(pl.multiple_of(z * width, width), width),
                ],
                dst_ref=returned.at[index * slots + slot],
                send_sem=back_out_sem.at[slot],
                recv_sem=back_in_sem.at[slot],
                device_id=(z, s),
                device_id_type=MESH,
            ).start()

        for z in planes_from(k):
            peers(k, z, send)
        returned[index * slots + slot] = u_ref[slot, my_rows, my_cols]

    def wait_return(sem):
        ref = returned.at[pl.ds(0, total - 1)]
        pltpu.make_async_copy(ref, ref, sem).wait()

    count = table_ref[2, 0]
    rate = (1.0 - decay_rate) / size

    def step(slot):
        live = slot < count
        g = g_ref[slot]
        left_old, right_old = factors[0, slot], factors[1, slot]
        left = decay_rate * left_old + rate * mm(g, g, 1, 1)
        right = decay_rate * right_old + rate * mm(g, g, 0, 0)
        nlf_ref[slot] = jnp.where(live, left, left_old)
        nrf_ref[slot] = jnp.where(live, right, right_old)
        left_root = root_of(left, (powers[0, 0, slot], powers[0, 1, slot]), roots[0, slot])
        nlr_ref[slot] = jnp.where(live, left_root, roots[0, slot])
        right_root = root_of(right, (powers[1, 0, slot], powers[1, 1, slot]), roots[1, slot])
        nrr_ref[slot] = jnp.where(live, right_root, roots[1, slot])
        hi, lo = split(left_root)
        product = split(mm(hi, g) + mm(lo, g))
        u_ref[slot] = mm3(product, split(right_root)).astype(bf16)

    @by_plane
    def _(k):
        for slot in range(slots):
            forward(slot, k)

    for slot in range(slots):
        by_plane(functools.partial(wait_forward, slot))
        step(slot)
        by_plane(functools.partial(backward, slot))
    for slot in range(slots):
        wait_return(back_in_sem.at[slot])
        wait_return(back_out_sem.at[slot])
        by_plane(functools.partial(wait_forward_sent, slot))
    for chunk in chunks:

        @pl.when(me != chunk[3])
        def _():
            hop(chunk, 1).wait_send()


def place_kernel(table, returned, *refs):
    news, out_ref, outs = refs[:4], refs[4], refs[5:9]
    acc, placed, table_ref, table_sem, sems, out_sem = refs[9:]
    table_copy = pltpu.make_async_copy(table, table_ref, table_sem)
    table_copy.start()
    copies = [
        pltpu.make_async_copy(new, out, sems.at[i])
        for i, (new, out) in enumerate(zip(news, outs))
    ]
    for copy in copies:
        copy.start()
    parts, _, cols, _ = out_ref.shape
    table_copy.wait()
    for b in range(parts):
        for c in range(cols):
            acc[b, :, c, :] = returned[table_ref[1, b * cols + c]].astype(f32)
        placed[b] = acc[b].astype(bf16)
        copies.append(pltpu.make_async_copy(placed.at[b], out_ref.at[b], out_sem.at[b]))
        copies[-1].start()
    for copy in copies:
        copy.wait()


def body(
    gradients, owner_list, row_offset, col_offset, left_factor, right_factor, left_root, right_root
):
    dp = lax.axis_size("dp")
    sh = lax.axis_size("shard")
    slots, size, _ = left_factor.shape
    _, parts, rows, cols, _ = gradients.shape
    width = size // dp
    total = dp * sh
    blocks = owner_list.shape[0]
    tall, owned = share_out(dp, rows)
    held = max(len(cells) for cells in owned) * tall
    hops = (dp, rows // tall, parts)
    lanes = -(-max(total * slots, blocks) // 128) * 128
    rowed = [x.reshape(1, blocks) for x in (owner_list, row_offset, col_offset)]

    vmem = pl.BlockSpec(memory_space=pltpu.VMEM)
    hbm = pl.BlockSpec(memory_space=pltpu.HBM)
    chunk = (dp, parts, rows, cols, width)
    matrices = (slots, size, size)
    dma = pltpu.SemaphoreType.DMA
    full = jax.ShapeDtypeStruct(matrices, f32)
    pieces = (total * slots, rows, width)
    table, returned, *news = pl.pallas_call(
        functools.partial(shampoo_kernel, dp, sh, slots),
        out_shape=[pltpu.VMEM((8, lanes), jnp.int32), pltpu.VMEM(pieces, bf16)] + [pltpu.VMEM(matrices, f32)] * 4,
        in_specs=[vmem] * 3 + [hbm] * 5,
        out_specs=[vmem] * 6,
        scratch_shapes=[
            pltpu.VMEM(chunk, bf16),
            pltpu.VMEM(chunk, bf16),
            pltpu.VMEM(chunk, bf16),
            pltpu.VMEM((tall, cols, width), f32),
            pltpu.VMEM((parts * cols, held, width), bf16),
            pltpu.VMEM((slots, total, held, width), bf16),
            pltpu.VMEM(matrices, bf16),
            pltpu.VMEM(matrices, bf16),
            pltpu.SMEM((8, lanes), jnp.int32),
            pltpu.VMEM((2,) + matrices, f32),
            pltpu.VMEM((2,) + matrices, f32),
            pltpu.VMEM((2, 2) + matrices, bf16),
            dma((dp, parts)), dma, dma((2,)), dma((2,)),
            dma(hops), dma(hops), dma(hops),
            dma((slots,)), dma((slots,)), dma((slots,)), dma((slots,)),
        ],
        compiler_params=pltpu.CompilerParams(
            collective_id=0, has_side_effects=True, vmem_limit_bytes=48 * 2**20
        ),
        name="shampoo",
    )(*rowed, gradients, left_factor, right_factor, left_root, right_root)
    return pl.pallas_call(
        place_kernel,
        out_shape=[jax.ShapeDtypeStruct((parts, rows, cols, width), bf16)] + [full] * 4,
        in_specs=[vmem] * 6,
        out_specs=[hbm] * 5,
        scratch_shapes=[
            pltpu.VMEM((parts, rows, cols, width), f32),
            pltpu.VMEM((parts, rows, cols, width), bf16),
            pltpu.SMEM((8, lanes), jnp.int32),
            dma, dma((4,)), dma((parts,)),
        ],
        compiler_params=pltpu.CompilerParams(vmem_limit_bytes=16 * 2**20),
        name="place",
    )(table, returned, *news)


def solution(mesh):
    owned = P(("dp", "shard"), None, None)
    in_specs = (P("dp", None, "shard", None, None), P(), P(), P(), owned, owned, owned, owned)
    out_specs = (P(None, "shard", None, "dp"), owned, owned, owned, owned)
    return jax.shard_map(body, mesh=mesh, in_specs=in_specs, out_specs=out_specs, check_vma=False)
```

```python
import functools

import jax
import jax.numpy as jnp
from jax import lax
from jax.experimental import pallas as pl
from jax.experimental.pallas import tpu as pltpu
from jax.sharding import PartitionSpec as P

decay_rate = 0.9
MESH = pl.DeviceIdType.MESH
f32 = jnp.float32
bf16 = jnp.bfloat16


def split(x):
    hi = x.astype(bf16)
    return hi, (x - hi.astype(f32)).astype(bf16)


def mm(a, b, ca=1, cb=0):
    return lax.dot_general(a, b, (((ca,), (cb,)), ((), ())), preferred_element_type=f32)


def mm3(a, b):
    return mm(a[0], b[0]) + (mm(a[0], b[1]) + mm(a[1], b[0]))


def root_of(factor, power, old_root):
    size = factor.shape[0]
    row = lax.broadcasted_iota(jnp.int32, factor.shape, 0)
    col = lax.broadcasted_iota(jnp.int32, factor.shape, 1)
    trace = jnp.sum(jnp.where(row == col, factor, 0.0))
    return 1.25 * old_root - mm3(power, split(factor)) * (size / (4.0 * trace))


def share_out(n, rows):
    tall = 32 if rows % 32 == 0 else rows
    cells = [(q, r) for q in range(n) for r in range(0, rows, tall)]
    shares = [len(cells) // n] * n
    if n == 4 and len(cells) % 8 == 0:
        shares = [len(cells) * 3 // 8, len(cells) // 8, len(cells) // 8, len(cells) * 3 // 8]
    starts = [sum(shares[:me]) for me in range(n)]
    return tall, [cells[at:at + share] for at, share in zip(starts, shares)]


def runs_of(cells, tall):
    runs = []
    for k, (q, r) in enumerate(cells):
        if runs and runs[-1][1] == q:
            runs[-1][3] += tall
        else:
            runs.append([k * tall, q, r, tall])
    return runs


def arrivals(owned, parts, latency=0.75):
    n = len(owned)
    events = {me: [] for me in range(n)}
    finals = {me: {} for me in range(n)}
    for step in (1, -1):
        line = list(range(n))[::step]
        ready = {(q, r, b, t): 0 for t in line[:0:-1] for q, r in owned[t] for b in range(parts)}
        for me in line:
            free = 0
            for chunk, at in sorted(ready.items(), key=lambda item: item[1]):
                if chunk[3] == me:
                    finals[me][chunk] = max(finals[me].get(chunk, 0), at)
                    del ready[chunk]
                else:
                    events[me].append((at, chunk, step))
                    free = max(free, at) + 1
                    ready[chunk] = free + latency
    return events, {me: sorted(finals[me], key=finals[me].get) for me in range(n)}


def build_table(index, slots, cols, size, owner_ref, row_ref, col_ref, table):
    blocks = owner_ref.shape[1]
    square = (blocks, blocks)
    row = lax.broadcasted_iota(jnp.int32, square, 0)
    col = lax.broadcasted_iota(jnp.int32, square, 1)

    def upright(x):
        return jnp.sum(jnp.where(row == col, x, 0), axis=1, keepdims=True)

    def total(pick, x):
        return jnp.sum(jnp.where(pick, x, 0), axis=0, keepdims=True)

    shift = size.bit_length() - 1
    owner = owner_ref[...]
    slot = owner * slots + total((upright(owner) == owner) & (row < col), 1)
    block = lax.shift_right_logical(row_ref[...], shift) * cols
    block = block + lax.shift_right_logical(col_ref[...], shift)
    slot, block = upright(slot), upright(block)
    lanes = table.shape[1]
    lane = lax.broadcasted_iota(jnp.int32, (blocks, lanes), 1)
    table[0:1] = total(slot == lane, block)
    table[1:2] = total(block == lane, slot)
    table[2:3] = total(upright(owner) == index, jnp.ones((blocks, lanes), jnp.int32))


def shampoo_kernel(n, sh, slots, owner_ref, row_ref, col_ref, grad_ref, lf_hbm, rf_hbm, lr_hbm, rr_hbm,
                   table, returned, nlf_ref, nrf_ref, nlr_ref, nrr_ref,
                   own, from_left, from_right, acc, pieces, packed, g_ref, u_ref, table_ref,
                   factors, roots, powers,
                   load_sem, table_sem, factor_sem, root_sem, send_sem, left_sem, right_sem,
                   out_sem, in_sem, back_out_sem, back_in_sem):
    me = lax.axis_index("dp")
    shard = lax.axis_index("shard")
    total = n * sh
    parts, rows, cols, width = own.shape[1:]
    size = g_ref.shape[1]
    tall, owned = share_out(n, rows)
    events, finals = arrivals(owned, parts)
    chunks = [(q, r, b, t) for t in range(n) for q, r in owned[t] for b in range(parts)]
    index = me * sh + shard
    barrier = pltpu.get_barrier_semaphore()

    @pl.when(me > 0)
    def _():
        pl.semaphore_signal(barrier, inc=1, device_id=(me - 1, shard), device_id_type=MESH)

    @pl.when(me < n - 1)
    def _():
        pl.semaphore_signal(barrier, inc=1, device_id=(me + 1, shard), device_id_type=MESH)

    @pl.loop(1, sh)
    def _(ds):
        pl.semaphore_signal(
            barrier, inc=1, device_id=(me, lax.rem(shard + ds, sh)), device_id_type=MESH
        )

    loads = {}
    order = []
    for j in range(n):
        for t in (n - 1 - j, j):
            if t not in order:
                order.append(t)
    for t in order:
        for b in range(parts):
            loads[t, b] = pltpu.make_async_copy(
                grad_ref.at[0, b, :, :, pl.ds(t * width, width)], own.at[t, b], load_sem.at[t, b]
            )
            loads[t, b].start()
    root_loads = [
        pltpu.make_async_copy(ref, roots.at[i], root_sem.at[i])
        for i, ref in enumerate((lr_hbm, rr_hbm))
    ]
    factor_loads = [
        pltpu.make_async_copy(ref, factors.at[i], factor_sem.at[i])
        for i, ref in enumerate((lf_hbm, rf_hbm))
    ]
    for copy in root_loads + factor_loads:
        copy.start()
    for t in order:
        for b in range(parts):
            loads[t, b].wait()
    beside = (me > 0).astype(jnp.int32) + (me < n - 1).astype(jnp.int32)
    pl.semaphore_wait(barrier, sh - 1 + beside)

    def place_of(chunk):
        q, r, b, _ = chunk
        return (q, b, pl.ds(r, tall)), (q, r // tall, b)

    def hop(chunk, step):
        buffer, sem = (from_left, left_sem) if step > 0 else (from_right, right_sem)
        at, sem_at = place_of(chunk)
        return pltpu.make_async_remote_copy(
            src_ref=own.at[at],
            dst_ref=buffer.at[at],
            send_sem=send_sem.at[sem_at],
            recv_sem=sem.at[sem_at],
            device_id=(me + step, shard),
            device_id_type=MESH,
        )

    units = [(i, s, part) for s in range(slots) for i in range(2) for part in range(3)]

    def next_power():
        if units:
            i, s, part = units.pop(0)
            if part == 0:
                x = split(roots[i, s])
                result = mm3(x, x)
            else:
                x = (powers[i, 0, s], powers[i, 1, s])
                result = mm3(x, x if part == 1 else split(roots[i, s]))
            powers[i, 0, s], powers[i, 1, s] = split(result)

    def pass_on(chunk, step):
        hop(chunk, step).wait_recv()
        buffer = from_left if step > 0 else from_right
        at, _ = place_of(chunk)
        own[at] = (own[at].astype(f32) + buffer[at].astype(f32)).astype(bf16)
        hop(chunk, step).start()

    def finish(k, chunk):
        at, _ = place_of(chunk)
        value = own[at].astype(f32)
        if k > 0:
            hop(chunk, 1).wait_recv()
            value = value + from_left[at].astype(f32)
        if k < n - 1:
            hop(chunk, -1).wait_recv()
            value = value + from_right[at].astype(f32)
        q, r, b, _ = chunk
        acc[...] = value
        first = owned[k].index((q, r)) * tall
        for c in range(cols):
            pieces[b * cols + c, first:first + tall] = acc[:, c, :].astype(bf16)

    def by_plane(visit):
        for k in range(n):
            pl.when(me == k)(functools.partial(visit, k))

    for end in (0, n - 1):

        @pl.when(me == end)
        def _():
            for _, chunk, step in events[end]:
                hop(chunk, step).start()

    build_table(index, slots, cols, size, owner_ref, row_ref, col_ref, table)
    table_copy = pltpu.make_async_copy(table, table_ref, table_sem)
    table_copy.start()
    for copy in root_loads:
        copy.wait()
    next_power()
    next_power()
    times = sorted({at for k in range(1, n - 1) for at, *_ in events[k]})
    pace = -(-len(units) // max(1, len(times) - 1))
    for now in times:
        for k in range(1, n - 1):
            arriving = [event for event in events[k] if event[0] == now]
            if arriving:

                @pl.when(me == k)
                def _():
                    for _, chunk, step in arriving:
                        pass_on(chunk, step)

        for _ in range(pace):
            next_power()
    while units:
        next_power()
    table_copy.wait()
    for copy in factor_loads:
        copy.wait()

    @by_plane
    def _(k):
        for chunk in finals[k]:
            finish(k, chunk)

    my_rows = pl.ds(pl.multiple_of(shard * rows, rows), rows)
    my_cols = pl.ds(pl.multiple_of(me * width, width), width)

    def planes_from(k):
        return sorted(range(n), key=lambda z: ((2 * z < n) == (2 * k < n), -abs(z - k)))

    def peers(k, z, visit):
        @pl.loop(1 if z == k else 0, sh)
        def _(ds):
            visit(z, lax.rem(shard + ds, sh))

    def forward(slot, k):
        tops = len(owned[k]) * tall

        def pack(z):
            @pl.loop(0, sh)
            def _(s):
                d = z * sh + s
                packed[slot, d, 0:tops] = pieces[table_ref[0, d * slots + slot], 0:tops]

        def block_part(q, r, high):
            return (
                slot,
                pl.ds(pl.multiple_of(shard * rows + r, tall), high),
                pl.ds(q * width, width),
            )

        def send(z, s):
            for top, q, r, high in runs_of(owned[k], tall):
                pltpu.make_async_remote_copy(
                    src_ref=packed.at[slot, z * sh + s, pl.ds(top, high)],
                    dst_ref=g_ref.at[block_part(q, r, high)],
                    send_sem=out_sem.at[slot],
                    recv_sem=in_sem.at[slot],
                    device_id=(z, s),
                    device_id_type=MESH,
                ).start()

        planes = planes_from(k)
        pack(planes[0])
        for z, following in zip(planes, planes[1:] + [None]):
            if following is not None:
                pack(following)
            peers(k, z, send)
        for top, q, r, high in runs_of(owned[k], tall):
            g_ref[block_part(q, r, high)] = packed[slot, index, pl.ds(top, high)]

    def wait_forward(slot, k):
        incoming = n * (size // tall) - len(owned[k])
        ref = returned.at[pl.ds(0, incoming), pl.ds(0, tall)]
        pltpu.make_async_copy(ref, ref, in_sem.at[slot]).wait()

    def wait_forward_sent(slot, k):
        ref = packed.at[slot, pl.ds(0, total - 1), pl.ds(0, len(owned[k]) * tall)]
        pltpu.make_async_copy(ref, ref, out_sem.at[slot]).wait()

    def backward(slot, k):
        def send(z, s):
            pltpu.make_async_remote_copy(
                src_ref=u_ref.at[
                    slot,
                    pl.ds(pl.multiple_of(s * rows, rows), rows),
                    pl.ds(pl.multiple_of(z * width, width), width),
                ],
                dst_ref=returned.at[index * slots + slot],
                send_sem=back_out_sem.at[slot],
                recv_sem=back_in_sem.at[slot],
                device_id=(z, s),
                device_id_type=MESH,
            ).start()

        for z in planes_from(k):
            peers(k, z, send)
        returned[index * slots + slot] = u_ref[slot, my_rows, my_cols]

    def wait_return(sem):
        ref = returned.at[pl.ds(0, total - 1)]
        pltpu.make_async_copy(ref, ref, sem).wait()

    count = table_ref[2, 0]
    rate = (1.0 - decay_rate) / size

    def step(slot):
        live = slot < count
        g = g_ref[slot]
        left_old, right_old = factors[0, slot], factors[1, slot]
        left = decay_rate * left_old + rate * mm(g, g, 1, 1)
        right = decay_rate * right_old + rate * mm(g, g, 0, 0)
        nlf_ref[slot] = jnp.where(live, left, left_old)
        nrf_ref[slot] = jnp.where(live, right, right_old)
        left_root = root_of(left, (powers[0, 0, slot], powers[0, 1, slot]), roots[0, slot])
        nlr_ref[slot] = jnp.where(live, left_root, roots[0, slot])
        right_root = root_of(right, (powers[1, 0, slot], powers[1, 1, slot]), roots[1, slot])
        nrr_ref[slot] = jnp.where(live, right_root, roots[1, slot])
        hi, lo = split(left_root)
        product = split(mm(hi, g) + mm(lo, g))
        u_ref[slot] = mm3(product, split(right_root)).astype(bf16)

    @by_plane
    def _(k):
        for slot in range(slots):
            forward(slot, k)

    for slot in range(slots):
        by_plane(functools.partial(wait_forward, slot))
        step(slot)
        by_plane(functools.partial(backward, slot))
    for slot in range(slots):
        wait_return(back_in_sem.at[slot])
        wait_return(back_out_sem.at[slot])
        by_plane(functools.partial(wait_forward_sent, slot))
    for chunk in chunks:

        @pl.when(me != chunk[3])
        def _():
            hop(chunk, 1).wait_send()


def place_kernel(table, returned, *refs):
    news, out_ref, outs = refs[:4], refs[4], refs[5:9]
    acc, placed, table_ref, table_sem, sems, out_sem = refs[9:]
    table_copy = pltpu.make_async_copy(table, table_ref, table_sem)
    table_copy.start()
    copies = [
        pltpu.make_async_copy(new, out, sems.at[i])
        for i, (new, out) in enumerate(zip(news, outs))
    ]
    for copy in copies:
        copy.start()
    parts, _, cols, _ = out_ref.shape
    table_copy.wait()
    for b in range(parts):
        for c in range(cols):
            acc[b, :, c, :] = returned[table_ref[1, b * cols + c]].astype(f32)
        placed[b] = acc[b].astype(bf16)
        copies.append(pltpu.make_async_copy(placed.at[b], out_ref.at[b], out_sem.at[b]))
        copies[-1].start()
    for copy in copies:
        copy.wait()


def body(
    gradients, owner_list, row_offset, col_offset, left_factor, right_factor, left_root, right_root
):
    dp = lax.axis_size("dp")
    sh = lax.axis_size("shard")
    slots, size, _ = left_factor.shape
    _, parts, rows, cols, _ = gradients.shape
    width = size // dp
    total = dp * sh
    blocks = owner_list.shape[0]
    tall, owned = share_out(dp, rows)
    held = max(len(cells) for cells in owned) * tall
    hops = (dp, rows // tall, parts)
    lanes = -(-max(total * slots, blocks) // 128) * 128
    rowed = [x.reshape(1, blocks) for x in (owner_list, row_offset, col_offset)]

    vmem = pl.BlockSpec(memory_space=pltpu.VMEM)
    hbm = pl.BlockSpec(memory_space=pltpu.HBM)
    chunk = (dp, parts, rows, cols, width)
    matrices = (slots, size, size)
    dma = pltpu.SemaphoreType.DMA
    full = jax.ShapeDtypeStruct(matrices, f32)
    pieces = (total * slots, rows, width)
    table, returned, *news = pl.pallas_call(
        functools.partial(shampoo_kernel, dp, sh, slots),
        out_shape=[pltpu.VMEM((8, lanes), jnp.int32), pltpu.VMEM(pieces, bf16)] + [pltpu.VMEM(matrices, f32)] * 4,
        in_specs=[vmem] * 3 + [hbm] * 5,
        out_specs=[vmem] * 6,
        scratch_shapes=[
            pltpu.VMEM(chunk, bf16),
            pltpu.VMEM(chunk, bf16),
            pltpu.VMEM(chunk, bf16),
            pltpu.VMEM((tall, cols, width), f32),
            pltpu.VMEM((parts * cols, held, width), bf16),
            pltpu.VMEM((slots, total, held, width), bf16),
            pltpu.VMEM(matrices, bf16),
            pltpu.VMEM(matrices, bf16),
            pltpu.SMEM((8, lanes), jnp.int32),
            pltpu.VMEM((2,) + matrices, f32),
            pltpu.VMEM((2,) + matrices, f32),
            pltpu.VMEM((2, 2) + matrices, bf16),
            dma((dp, parts)), dma, dma((2,)), dma((2,)),
            dma(hops), dma(hops), dma(hops),
            dma((slots,)), dma((slots,)), dma((slots,)), dma((slots,)),
        ],
        compiler_params=pltpu.CompilerParams(
            collective_id=0, has_side_effects=True, vmem_limit_bytes=48 * 2**20
        ),
        name="shampoo",
    )(*rowed, gradients, left_factor, right_factor, left_root, right_root)
    return pl.pallas_call(
        place_kernel,
        out_shape=[jax.ShapeDtypeStruct((parts, rows, cols, width), bf16)] + [full] * 4,
        in_specs=[vmem] * 6,
        out_specs=[hbm] * 5,
        scratch_shapes=[
            pltpu.VMEM((parts, rows, cols, width), f32),
            pltpu.VMEM((parts, rows, cols, width), bf16),
            pltpu.SMEM((8, lanes), jnp.int32),
            dma, dma((4,)), dma((parts,)),
        ],
        compiler_params=pltpu.CompilerParams(vmem_limit_bytes=16 * 2**20),
        name="place",
    )(table, returned, *news)


def solution(mesh):
    owned = P(("dp", "shard"), None, None)
    in_specs = (P("dp", None, "shard", None, None), P(), P(), P(), owned, owned, owned, owned)
    out_specs = (P(None, "shard", None, "dp"), owned, owned, owned, owned)
    return jax.shard_map(body, mesh=mesh, in_specs=in_specs, out_specs=out_specs, check_vma=False)
```
